32 devices in a mesh: data: 2 (over x), expert: 16 (over z, y, core).
Axes of the slice: x: 2, y: 2, z: 4, core: 2. Of those that a mesh axis runs over, the one named last changes fastest.
Arguments:
- x_in: bfloat16 [32768, 512], P(('data', 'expert')), parts along dimension 0
- expert_idx: int32 [32768, 8], P(('data', 'expert')), parts along dimension 0
- gate_weight: float32 [32768, 8], P(('data', 'expert')), parts along dimension 0
- grad_y: bfloat16 [32768, 512], P(('data', 'expert')), parts along dimension 0
- w_in: bfloat16 [64, 512, 256], P('expert')
- w_out: bfloat16 [64, 256, 512], P('expert')
Outputs:
- output 1: bfloat16 [32768, 512], P(('data', 'expert')), parts along dimension 0
- output 2: bfloat16 [32768, 512], P(('data', 'expert')), parts along dimension 0
- output 3: float32 [32768, 8], P(('data', 'expert')), parts along dimension 0
- output 4: bfloat16 [128, 512, 256], P(('data', 'expert')), parts along dimension 0
- output 5: bfloat16 [128, 256, 512], P(('data', 'expert')), parts along dimension 0
There are 2 independent parts. The reference program is written for one: setup_inputs(seed, part) draws one part's arguments, and reference() takes and returns one part's arrays. A program takes and returns all parts, laid end to end along the dimension named above; an argument that names none is the same for every part.
All inputs are finite; a program needn't handle non-finite values.
Results may differ from the reference program's by a relative error of at most 0.0100954.
Values are sent between devices in bfloat16 or wider.
A program may use at most 1 GiB of HBM per device.

```python
import jax
import jax.numpy as jnp
from jax import lax

TOKENS = 1024
GROUP_SIZE = 16
D_MODEL = 512
D_FF = 256
EXPERTS = 64
TOP_K = 8
CAPACITY = 2560

LOCAL_EXPERTS = EXPERTS // GROUP_SIZE
DEVICE_PAIRS = TOKENS * TOP_K
FAIR_SHARE = DEVICE_PAIRS // GROUP_SIZE
GROUP_ROWS = GROUP_SIZE * TOKENS
GROUP_PAIRS = GROUP_ROWS * TOP_K


def route_device(rng_key, hot_offset):
    key_perm, key_shift, key_quartet, key_pick, key_shuffle = jax.random.split(rng_key, 5)
    owner_perm = jax.random.permutation(key_perm, GROUP_SIZE)
    shift_size = jax.random.randint(key_shift, (GROUP_SIZE // 2,), 0, FAIR_SHARE + 1)
    shift_size = shift_size.at[0].set(FAIR_SHARE)
    per_owner = jnp.full((GROUP_SIZE,), FAIR_SHARE, jnp.int32)
    per_owner = per_owner.at[owner_perm[0::2]].add(shift_size).at[owner_perm[1::2]].add(-shift_size)
    owner_dev = jnp.searchsorted(jnp.cumsum(per_owner), jnp.arange(DEVICE_PAIRS, dtype=jnp.int32), side='right')
    quartet = jax.random.randint(key_quartet, (DEVICE_PAIRS,), 0, LOCAL_EXPERTS // 4)
    pick_draw = jax.random.randint(key_pick, (DEVICE_PAIRS,), 0, 8)
    hot_slot = hot_offset[owner_dev, quartet]
    within = jnp.where(pick_draw < 5, hot_slot, (hot_slot + pick_draw - 4) % 4)
    expert_id = owner_dev * LOCAL_EXPERTS + quartet * 4 + within
    return expert_id[jax.random.permutation(key_shuffle, DEVICE_PAIRS)].astype(jnp.int32)


def setup_inputs(seed: int = 0, part: int = 0) -> dict:
    part_key = jax.random.fold_in(jax.random.key(seed), part)
    key_x, key_gate, key_dy, key_hot, key_route = jax.random.split(part_key, 5)
    key_in, key_out = jax.random.split(jax.random.key(seed + 1), 2)
    hot_offset = jax.random.randint(key_hot, (GROUP_SIZE, LOCAL_EXPERTS // 4), 0, 4)
    route_keys = jax.random.split(key_route, GROUP_SIZE)
    expert_idx = jax.vmap(route_device, in_axes=(0, None))(route_keys, hot_offset).reshape(GROUP_ROWS, TOP_K)
    x_in = jax.random.normal(key_x, (GROUP_ROWS, D_MODEL), jnp.float32).astype(jnp.bfloat16)
    gate_weight = jax.random.uniform(key_gate, (GROUP_ROWS, TOP_K), jnp.float32, 0.5, 1.5) * TOP_K ** -0.5
    grad_y = jax.random.normal(key_dy, (GROUP_ROWS, D_MODEL), jnp.float32).astype(jnp.bfloat16)
    w_in = (jax.random.normal(key_in, (EXPERTS, D_MODEL, D_FF), jnp.float32) * D_MODEL ** -0.5).astype(jnp.bfloat16)
    w_out = (jax.random.normal(key_out, (EXPERTS, D_FF, D_MODEL), jnp.float32) * D_FF ** -0.5).astype(jnp.bfloat16)
    return {'x_in': x_in, 'expert_idx': expert_idx, 'gate_weight': gate_weight, 'grad_y': grad_y, 'w_in': w_in, 'w_out': w_out}


def reference(x_in, expert_idx, gate_weight, grad_y, w_in, w_out):
    flat_idx = expert_idx.reshape(GROUP_PAIRS)
    pair_ids = jnp.arange(GROUP_PAIRS, dtype=jnp.int32)
    sort_order = jnp.argsort(flat_idx, stable=True)
    counts = jnp.zeros((EXPERTS,), jnp.int32).at[flat_idx].add(1)
    starts = jnp.cumsum(counts) - counts
    sorted_rank = pair_ids - starts[flat_idx[sort_order]]
    pair_slot = jnp.zeros((GROUP_PAIRS,), jnp.int32).at[sort_order].set(sorted_rank)
    dest_row = jnp.where(pair_slot < CAPACITY, flat_idx * CAPACITY + pair_slot, EXPERTS * CAPACITY)
    source_pair = jnp.full((EXPERTS * CAPACITY,), GROUP_PAIRS, jnp.int32).at[dest_row].set(pair_ids, mode='drop')
    exp_rows = jnp.take(x_in, source_pair // TOP_K, axis=0, mode='fill', fill_value=0).reshape(EXPERTS, CAPACITY, D_MODEL)
    scaled_grad = (gate_weight[:, :, None] * grad_y[:, None, :].astype(jnp.float32)).astype(jnp.bfloat16).reshape(GROUP_PAIRS, D_MODEL)
    grad_rows = jnp.take(scaled_grad, source_pair, axis=0, mode='fill', fill_value=0).reshape(EXPERTS, CAPACITY, D_MODEL)

    def expert_pass(operands):
        rows_in, rows_grad, weight_in, weight_out = operands
        pre_act = jnp.dot(rows_in, weight_in, preferred_element_type=jnp.float32)
        act_full, gelu_pull = jax.vjp(jax.nn.gelu, pre_act)
        act_bf = act_full.astype(jnp.bfloat16)
        rows_out = jnp.dot(act_bf, weight_out, preferred_element_type=jnp.float32).astype(jnp.bfloat16)
        grad_act = jnp.dot(rows_grad, weight_out.T, preferred_element_type=jnp.float32).astype(jnp.bfloat16)
        grad_pre = gelu_pull(grad_act.astype(jnp.float32))[0].astype(jnp.bfloat16)
        grad_weight_out = jnp.dot(act_bf.T, rows_grad, preferred_element_type=jnp.float32).astype(jnp.bfloat16)
        grad_weight_in = jnp.dot(rows_in.T, grad_pre, preferred_element_type=jnp.float32).astype(jnp.bfloat16)
        grad_in = jnp.dot(grad_pre, weight_in.T, preferred_element_type=jnp.float32).astype(jnp.bfloat16)
        return rows_out, grad_in, grad_weight_in, grad_weight_out

    out_rows, grad_in_rows, grad_w_in, grad_w_out = lax.map(expert_pass, (exp_rows, grad_rows, w_in, w_out))
    out_pair = jnp.take(out_rows.reshape(EXPERTS * CAPACITY, D_MODEL), dest_row, axis=0, mode='fill', fill_value=0).reshape(GROUP_ROWS, TOP_K, D_MODEL).astype(jnp.float32)
    grad_pair = jnp.take(grad_in_rows.reshape(EXPERTS * CAPACITY, D_MODEL), dest_row, axis=0, mode='fill', fill_value=0).reshape(GROUP_ROWS, TOP_K, D_MODEL).astype(jnp.float32)
    y_out = (x_in.astype(jnp.float32) + jnp.sum(gate_weight[:, :, None] * out_pair, axis=1)).astype(jnp.bfloat16)
    grad_gate = jnp.sum(grad_y.astype(jnp.float32)[:, None, :] * out_pair, axis=2)
    grad_x = (grad_y.astype(jnp.float32) + jnp.sum(grad_pair, axis=1)).astype(jnp.bfloat16)
    return y_out, grad_x, grad_gate, grad_w_in, grad_w_out
```

```python
import functools

import jax
import jax.numpy as jnp
from jax import lax
from jax.experimental import pallas as pl
from jax.experimental.pallas import tpu as pltpu
from jax.sharding import PartitionSpec as P

CAP_NUM = 5
CAP_DEN = 4
PAIR_FACTOR = 2

TILE = 128
ALIGN = 8
LANES = 128
TOKENS_PER_STEP = 16
VMEM_BYTES = 62 * 1024 * 1024
GELU_C = 0.7978845608028654
GELU_K = 0.044715


def ceil_to(n, m):
    return (n + m - 1) // m * m


def gelu_parts(a):
    sq = a * a
    t = jnp.tanh(GELU_C * (a + GELU_K * (sq * a)))
    cdf = 0.5 * (1.0 + t)
    slope = cdf + (0.5 * a) * (1.0 - t * t) * (GELU_C * (1.0 + (3.0 * GELU_K) * sq))
    return a * cdf, slope


def dot_nn(a, b):
    return jnp.dot(a, b, preferred_element_type=jnp.float32)


def dot_nt(a, b):
    return lax.dot_general(a, b, (((1,), (1,)), ((), ())), preferred_element_type=jnp.float32)


def dot_tn(a, b):
    return lax.dot_general(a, b, (((0,), (0,)), ((), ())), preferred_element_type=jnp.float32)


def pick_matrix(meta, n_tokens):
    tok = meta[:, 0:1].astype(jnp.int32)
    cols = lax.broadcasted_iota(jnp.int32, (meta.shape[0], n_tokens), 1)
    return jnp.where(tok == cols, 1.0, 0.0).astype(jnp.bfloat16)


def token_kernel(zero_row, top_k, sc_ref, pos_ref, meta_ref, x_ref, dy_ref, w1_ref, w2_ref,
                 y_ref, dx_ref, dg_ref, buf, dgb, tmp, tmpg):
    e = pl.program_id(0)
    n_tokens, d = x_ref.shape

    @pl.when(e == 0)
    def _():
        buf[pl.ds(zero_row, ALIGN), :] = jnp.zeros((ALIGN, 2 * d), jnp.float32)
        dgb[pl.ds(zero_row, ALIGN), :] = jnp.zeros((ALIGN, LANES), jnp.float32)

    list_start, buf_start, kept = sc_ref[0, e], sc_ref[1, e], sc_ref[2, e]

    def tile(i, carry):
        meta = meta_ref[pl.ds(pl.multiple_of(list_start + i * TILE, ALIGN), TILE), :]
        pick = pick_matrix(meta, n_tokens)
        gate = meta[:, 1:2]
        rows = dot_nn(pick, x_ref[...]).astype(jnp.bfloat16)
        drow = dot_nn(pick, dy_ref[...])
        act, slope = gelu_parts(dot_nn(rows, w1_ref[0]))
        out = dot_nn(act.astype(jnp.bfloat16), w2_ref[0]).astype(jnp.bfloat16).astype(jnp.float32)
        grad = (gate * drow).astype(jnp.bfloat16)
        dact = dot_nt(grad, w2_ref[0]).astype(jnp.bfloat16).astype(jnp.float32)
        dpre = (dact * slope).astype(jnp.bfloat16)
        din = dot_nt(dpre, w1_ref[0]).astype(jnp.bfloat16).astype(jnp.float32)
        at = pl.ds(pl.multiple_of(buf_start + i * TILE, ALIGN), TILE)
        buf[at, 0:d] = gate * out
        buf[at, d:2 * d] = din
        dgb[at, :] = jnp.broadcast_to(jnp.sum(drow * out, axis=1, keepdims=True), (TILE, LANES))
        return carry

    lax.fori_loop(0, (kept + TILE - 1) // TILE, tile, 0)

    @pl.when(e == pl.num_programs(0) - 1)
    def _():
        lane = lax.broadcasted_iota(jnp.int32, (1, LANES), 1)

        def block(b, carry):
            for k in range(TOKENS_PER_STEP):
                acc, dg = None, jnp.zeros((1, LANES), jnp.float32)
                for j in range(top_k):
                    r = pos_ref[(b * TOKENS_PER_STEP + k) * top_k + j]
                    row = buf[pl.ds(r, 1), :]
                    acc = row if acc is None else acc + row
                    dg = jnp.where(lane == j, dgb[pl.ds(r, 1), :], dg)
                tmp[k:k + 1, :] = acc
                tmpg[k:k + 1, :] = dg
            at = pl.ds(pl.multiple_of(b * TOKENS_PER_STEP, TOKENS_PER_STEP), TOKENS_PER_STEP)
            y_ref[at, :] = (x_ref[at, :].astype(jnp.float32) + tmp[:, 0:d]).astype(jnp.bfloat16)
            dx_ref[at, :] = (dy_ref[at, :].astype(jnp.float32) + tmp[:, d:2 * d]).astype(jnp.bfloat16)
            dg_ref[at, :] = tmpg[...]
            return carry

        lax.fori_loop(0, n_tokens // TOKENS_PER_STEP, block, 0)


def token_pass(scalars, pos, meta, block_rows, x, dy, w1, w2, buf_rows, zero_row, top_k):
    n_tokens, d = x.shape
    experts, _, f = w1.shape
    per_dev = experts * block_rows // meta.shape[0]
    whole = lambda e, *_: (0, 0)
    return pl.pallas_call(
        functools.partial(token_kernel, zero_row, top_k),
        out_shape=(jax.ShapeDtypeStruct((n_tokens, d), jnp.bfloat16),
                   jax.ShapeDtypeStruct((n_tokens, d), jnp.bfloat16),
                   jax.ShapeDtypeStruct((n_tokens, LANES), jnp.float32)),
        grid_spec=pltpu.PrefetchScalarGridSpec(
            num_scalar_prefetch=2, grid=(experts,),
            in_specs=[pl.BlockSpec((block_rows, 2), lambda e, *_: (e // per_dev, 0)),
                      pl.BlockSpec((n_tokens, d), whole, pipeline_mode=pl.Buffered(1)),
                      pl.BlockSpec((n_tokens, d), whole, pipeline_mode=pl.Buffered(1)),
                      pl.BlockSpec((1, d, f), lambda e, *_: (e, 0, 0)),
                      pl.BlockSpec((1, f, d), lambda e, *_: (e, 0, 0))],
            out_specs=[pl.BlockSpec((n_tokens, d), whole, pipeline_mode=pl.Buffered(1)),
                       pl.BlockSpec((n_tokens, d), whole, pipeline_mode=pl.Buffered(1)),
                       pl.BlockSpec((n_tokens, LANES), whole, pipeline_mode=pl.Buffered(1))],
            scratch_shapes=[pltpu.VMEM((buf_rows, 2 * d), jnp.float32),
                            pltpu.VMEM((buf_rows, LANES), jnp.float32),
                            pltpu.VMEM((TOKENS_PER_STEP, 2 * d), jnp.float32),
                            pltpu.VMEM((TOKENS_PER_STEP, LANES), jnp.float32)]),
        compiler_params=pltpu.CompilerParams(dimension_semantics=("arbitrary",), vmem_limit_bytes=VMEM_BYTES),
        cost_estimate=pl.CostEstimate(flops=60_000_000_000, bytes_accessed=40_000_000, transcendentals=4_000_000),
        name="token_pass",
    )(scalars, pos, meta, x, dy, w1, w2)


def owner_kernel(sc_ref, meta_ref, x_ref, dy_ref, w1_ref, w2_ref, dw1_ref, dw2_ref, acc1, acc2):
    s = pl.program_id(0)
    n_tokens, d = x_ref.shape
    local_experts = w1_ref.shape[0]

    @pl.when(s == 0)
    def _():
        acc1[...] = jnp.zeros_like(acc1)
        acc2[...] = jnp.zeros_like(acc2)

    for e in range(local_experts):
        start, kept = sc_ref[0, s * local_experts + e], sc_ref[1, s * local_experts + e]

        def tile(i, carry, e=e, start=start, kept=kept):
            meta = meta_ref[pl.ds(pl.multiple_of(start + i * TILE, ALIGN), TILE), :]
            pick = pick_matrix(meta, n_tokens)
            live = lax.broadcasted_iota(jnp.int32, (TILE, 1), 0) + i * TILE < kept
            gate = jnp.where(live, meta[:, 1:2], 0.0)
            rows = dot_nn(pick, x_ref[...]).astype(jnp.bfloat16)
            grad = (gate * dot_nn(pick, dy_ref[...])).astype(jnp.bfloat16)
            act, slope = gelu_parts(dot_nn(rows, w1_ref[e]))
            dact = dot_nt(grad, w2_ref[e]).astype(jnp.bfloat16).astype(jnp.float32)
            dpre = (dact * slope).astype(jnp.bfloat16)
            acc2[e] += dot_tn(act.astype(jnp.bfloat16), grad)
            acc1[e] += dot_tn(rows, dpre)
            return carry

        lax.fori_loop(0, (kept + TILE - 1) // TILE, tile, 0)

    @pl.when(s == pl.num_programs(0) - 1)
    def _():
        dw1_ref[...] = acc1[...].astype(jnp.bfloat16)
        dw2_ref[...] = acc2[...].astype(jnp.bfloat16)


def owner_pass(scalars, meta, x_all, dy_all, w1, w2, sources):
    local_experts, d, f = w1.shape
    n_tokens = x_all.shape[0] // sources
    block_rows = meta.shape[0] // sources
    return pl.pallas_call(
        owner_kernel,
        out_shape=(jax.ShapeDtypeStruct(w1.shape, jnp.bfloat16), jax.ShapeDtypeStruct(w2.shape, jnp.bfloat16)),
        grid_spec=pltpu.PrefetchScalarGridSpec(
            num_scalar_prefetch=1, grid=(sources,),
            in_specs=[pl.BlockSpec((block_rows, 2), lambda s, *_: (s, 0)),
                      pl.BlockSpec((n_tokens, d), lambda s, *_: (s, 0)),
                      pl.BlockSpec((n_tokens, d), lambda s, *_: (s, 0)),
                      pl.BlockSpec(w1.shape, lambda s, *_: (0, 0, 0)),
                      pl.BlockSpec(w2.shape, lambda s, *_: (0, 0, 0))],
            out_specs=[pl.BlockSpec(w1.shape, lambda s, *_: (0, 0, 0)),
                       pl.BlockSpec(w2.shape, lambda s, *_: (0, 0, 0))],
            scratch_shapes=[pltpu.VMEM(w1.shape, jnp.float32), pltpu.VMEM(w2.shape, jnp.float32)]),
        compiler_params=pltpu.CompilerParams(dimension_semantics=("arbitrary",), vmem_limit_bytes=VMEM_BYTES // 2),
        cost_estimate=pl.CostEstimate(flops=50_000_000_000, bytes_accessed=50_000_000, transcendentals=3_000_000),
        name="owner_pass",
    )(scalars, meta, x_all, dy_all, w1, w2)


def split3(v):
    a = lax.reduce_precision(v, 8, 7)
    b = lax.reduce_precision(v - a, 8, 7)
    return a, b, lax.reduce_precision(v - a - b, 8, 7)


def route(expert_idx, gate, num_experts, groups, list_rows):
    n_tokens, top_k = expert_idx.shape
    n_pairs = n_tokens * top_k
    local_experts = num_experts // groups
    chunk = 256
    flat = expert_idx.reshape(n_pairs)
    hot = (flat[:, None] == jnp.arange(num_experts, dtype=jnp.int32)[None, :])
    hot_b = hot.astype(jnp.bfloat16).reshape(n_pairs // chunk, chunk, num_experts)
    lower = jnp.tril(jnp.ones((chunk, chunk), jnp.bfloat16), -1)
    inner = jnp.einsum('ij,bje->bie', lower, hot_b, preferred_element_type=jnp.float32)
    sums = jnp.sum(hot_b.astype(jnp.float32), axis=1)
    through = jnp.cumsum(sums, axis=0)
    ranks = inner + (through - sums)[:, None, :]
    counts = through[-1].astype(jnp.int32)
    padded = (counts + ALIGN - 1) // ALIGN * ALIGN
    grid = padded.reshape(groups, local_experts)
    local_start = (jnp.cumsum(grid, axis=1) - grid).reshape(num_experts)
    list_start = local_start + jnp.repeat(jnp.arange(groups, dtype=jnp.int32) * list_rows, local_experts)
    rank = jnp.sum(hot_b.astype(jnp.float32) * ranks, axis=2).reshape(n_pairs).astype(jnp.int32)
    start_of = jnp.sum(jnp.where(hot, list_start[None, :], 0), axis=1)
    list_pos = start_of + rank
    hi = (list_pos[:, None] // LANES == jnp.arange(groups * list_rows // LANES, dtype=jnp.int32)[None, :]).astype(jnp.bfloat16)
    lo = list_pos[:, None] % LANES == jnp.arange(LANES, dtype=jnp.int32)[None, :]
    token = jnp.arange(n_pairs, dtype=jnp.int32) // top_k
    parts = [(token // 32).astype(jnp.float32), (token % 32).astype(jnp.float32), *split3(gate.reshape(n_pairs))]
    vals = jnp.concatenate([jnp.where(lo, v[:, None], 0.0).astype(jnp.bfloat16) for v in parts], axis=1)
    lists = lax.dot_general(hi, vals, (((0,), (0,)), ((), ())), preferred_element_type=jnp.float32)
    t_hi, t_lo, g1, g2, g3 = (lists[:, k * LANES:(k + 1) * LANES] for k in range(5))
    return flat, hot, rank, counts, padded, local_start, 32.0 * t_hi + t_lo, g1 + g2 + g3


def columns(tokens, gates):
    return jnp.stack([tokens.reshape(-1), gates.reshape(-1)], axis=1)


def solution(mesh):
    groups = mesh.shape['expert']
    tok_spec = P(('data', 'expert'), None)
    weight_spec = P('expert', None, None)
    grad_spec = P(('data', 'expert'), None, None)

    def device_pass(x_in, expert_idx, gate_weight, grad_y, w_in, w_out):
        n_tokens, top_k = expert_idx.shape
        local_experts = w_in.shape[0]
        num_experts = local_experts * groups
        n_pairs = n_tokens * top_k
        capacity = (CAP_NUM * n_pairs * groups) // (CAP_DEN * num_experts)
        pair_cap = PAIR_FACTOR * n_pairs // groups
        list_rows = ceil_to(pair_cap + local_experts * (ALIGN - 1) + TILE, LANES)
        me = lax.axis_index('expert')

        w1_all = lax.all_gather(w_in, 'expert', axis=0, tiled=True)
        w2_all = lax.all_gather(w_out, 'expert', axis=0, tiled=True)

        flat, hot, rank, counts, padded, local_start, tok_list, gate_list = route(
            expert_idx, gate_weight, num_experts, groups, list_rows)
        counts_all = lax.all_gather(counts, 'expert')
        before = jnp.cumsum(counts_all, axis=0) - counts_all
        kept_all = jnp.clip(capacity - before, 0, counts_all)
        kept_mine = lax.dynamic_index_in_dim(kept_all, me, 0, keepdims=False)

        buf_start = jnp.cumsum(padded) - padded
        zero_row = n_pairs + num_experts * (ALIGN - 1) + TILE
        buf_rows = zero_row + ALIGN
        pick = lambda v: jnp.sum(jnp.where(hot, v[None, :], 0), axis=1)
        pos = jnp.where(rank < pick(kept_mine), pick(buf_start) + rank, zero_row)
        token_scalars = jnp.stack([local_start, buf_start, kept_mine])
        y_out, grad_x, grad_gate = token_pass(token_scalars, pos, columns(tok_list, gate_list), list_rows,
                                              x_in, grad_y, w1_all, w2_all, buf_rows, zero_row, top_k)

        grid_all = ((counts_all + ALIGN - 1) // ALIGN * ALIGN).reshape(groups, groups, local_experts)
        start_all = jnp.cumsum(grid_all, axis=2) - grid_all
        start_own = lax.dynamic_index_in_dim(start_all, me, 1, keepdims=False).reshape(-1)
        kept_own = lax.dynamic_index_in_dim(kept_all.reshape(groups, groups, local_experts), me, 1, keepdims=False).reshape(-1)
        lists = jnp.stack([tok_list.reshape(groups, -1, LANES), gate_list.reshape(groups, -1, LANES)], axis=1)
        lists = lax.all_to_all(lists, 'expert', 0, 0, tiled=True)
        x_all = lax.all_gather(x_in, 'expert', axis=0, tiled=True)
        dy_all = lax.all_gather(grad_y, 'expert', axis=0, tiled=True)
        grad_w_in, grad_w_out = owner_pass(jnp.stack([start_own, kept_own]), columns(lists[:, 0], lists[:, 1]),
                                           x_all, dy_all, w_in, w_out, groups)
        return y_out, grad_x, grad_gate[:, :top_k], grad_w_in, grad_w_out

    return jax.shard_map(device_pass, mesh=mesh,
                         in_specs=(tok_spec, tok_spec, tok_spec, tok_spec, weight_spec, weight_spec),
                         out_specs=(tok_spec, tok_spec, tok_spec, grad_spec, grad_spec), check_vma=False)
```

```python
import functools

import jax
import jax.numpy as jnp
from jax import lax
from jax.experimental import pallas as pl
from jax.experimental.pallas import tpu as pltpu
from jax.sharding import PartitionSpec as P


CAP_NUM = 5
CAP_DEN = 4
PAIR_FACTOR = 2

TILE = 128
PICK_TILE = 256
TOKEN_UNROLL = 2
OWNER_UNROLL = 2
ALIGN = 16
LANES = 128
TOKENS_PER_STEP = 16
VMEM_BYTES = 62 * 1024 * 1024
GELU_C = 0.7978845608028654
GELU_K = 0.044715


def ceil_to(n, m):
    return (n + m - 1) // m * m


def gelu_parts(a):
    sq = a * a
    t = jnp.tanh(GELU_C * (a + GELU_K * (sq * a)))
    cdf = 0.5 * (1.0 + t)
    slope = cdf + (0.5 * a) * (1.0 - t * t) * (GELU_C * (1.0 + (3.0 * GELU_K) * sq))
    return a * cdf, slope


def dot_nn(a, b):
    return jnp.dot(a, b, preferred_element_type=jnp.float32)


def dot_nt(a, b):
    return lax.dot_general(a, b, (((1,), (1,)), ((), ())), preferred_element_type=jnp.float32)


def dot_tn(a, b):
    return lax.dot_general(a, b, (((0,), (0,)), ((), ())), preferred_element_type=jnp.float32)


def pick_matrix(meta, n_tokens):
    tok = meta[:, 0:1].astype(jnp.int32)
    cols = lax.broadcasted_iota(jnp.int32, (meta.shape[0], n_tokens), 1)
    return jnp.where(tok == cols, 1.0, 0.0).astype(jnp.bfloat16)


def pick_kernel(n_ref, meta_ref, x_ref, dy_ref, rows_ref, drow_ref):
    used = n_ref[pl.program_id(0)]

    def tile(i, carry):
        at = pl.ds(pl.multiple_of(i * PICK_TILE, PICK_TILE), PICK_TILE)
        pick = pick_matrix(meta_ref[at, :], x_ref.shape[0])
        rows_ref[at, :] = dot_nn(pick, x_ref[...]).astype(jnp.bfloat16)
        drow_ref[at, :] = dot_nn(pick, dy_ref[...]).astype(jnp.bfloat16)
        return carry

    lax.fori_loop(0, (used + PICK_TILE - 1) // PICK_TILE, tile, 0)


def pick_pass(used, meta, x, dy):
    n_tokens, d = x.shape
    dests = used.shape[0]
    block_rows = meta.shape[0] // dests
    whole = lambda e, *_: (0, 0)
    row = lambda e, *_: (e, 0)
    out = jax.ShapeDtypeStruct((meta.shape[0], d), jnp.bfloat16)
    return pl.pallas_call(
        pick_kernel,
        out_shape=(out, out),
        grid_spec=pltpu.PrefetchScalarGridSpec(
            num_scalar_prefetch=1, grid=(dests,),
            in_specs=[pl.BlockSpec((block_rows, 2), row),
                      pl.BlockSpec((n_tokens, d), whole), pl.BlockSpec((n_tokens, d), whole)],
            out_specs=[pl.BlockSpec((block_rows, d), row), pl.BlockSpec((block_rows, d), row)]),
        compiler_params=pltpu.CompilerParams(dimension_semantics=("arbitrary",), vmem_limit_bytes=VMEM_BYTES // 2),
        cost_estimate=pl.CostEstimate(flops=20_000_000_000, bytes_accessed=50_000_000, transcendentals=0),
        name="pick_pass",
    )(used, meta, x, dy)


def out_product(act, w):
    f = w.shape[1]
    d = 2 * f
    return jnp.concatenate([dot_nn(act, w[d:d + f, :]), dot_nn(act, w[d + f:d + 2 * f, :])], axis=1)


def out_product_t(grad, w):
    f = w.shape[1]
    d = 2 * f
    return dot_nt(grad[:, 0:f], w[d:d + f, :]) + dot_nt(grad[:, f:d], w[d + f:d + 2 * f, :])


def tile_table(kept):
    ends, total = [], 0
    for k in kept:
        total = total + (k + TILE - 1) // TILE
        ends.append(total)

    def find(i):
        e, base, live_from = jnp.int32(0), jnp.int32(0), kept[0]
        for n in range(1, len(kept)):
            past = i >= ends[n - 1]
            e = jnp.where(past, n, e)
            base = jnp.where(past, ends[n - 1], base)
            live_from = jnp.where(past, kept[n], live_from)
        off = (i - base) * TILE
        return e, off, live_from - off

    return total, find


def token_kernel(zero_row, top_k, sc_ref, src_ref, pos_ref, meta_ref, rows_ref, drow_ref, x_ref, dy_ref, w_ref,
                 y_ref, dx_ref, dg_ref, buf, dgb, tmp, tmpg):
    g = pl.program_id(0)
    n_tokens, d = x_ref.shape
    local_experts = w_ref.shape[0]
    spare_row = zero_row + ALIGN

    @pl.when(g == 0)
    def _():
        buf[pl.ds(zero_row, ALIGN), :] = jnp.zeros((ALIGN, 2 * d), jnp.float32)
        dgb[pl.ds(zero_row, ALIGN), :] = jnp.zeros((ALIGN, LANES), jnp.float32)

    first = g * local_experts
    total, find = tile_table([sc_ref[2, first + n] for n in range(local_experts)])

    def tiles(p, carry):
        for u in range(TOKEN_UNROLL):
            e, off, live = find(p * TOKEN_UNROLL + u)
            real = live > 0
            at = pl.ds(pl.multiple_of(jnp.where(real, sc_ref[0, first + e] + off, 0), ALIGN), TILE)
            w = w_ref.at[e]
            gate = meta_ref[at, 1:2]
            drow = drow_ref[at, :].astype(jnp.float32)
            act, slope = gelu_parts(dot_nn(rows_ref[at, :], w[0:d, :]))
            out = out_product(act.astype(jnp.bfloat16), w).astype(jnp.bfloat16).astype(jnp.float32)
            grad = (gate * drow).astype(jnp.bfloat16)
            dact = out_product_t(grad, w).astype(jnp.bfloat16).astype(jnp.float32)
            dpre = (dact * slope).astype(jnp.bfloat16)
            din = dot_nt(dpre, w[0:d, :]).astype(jnp.bfloat16).astype(jnp.float32)
            at = pl.ds(pl.multiple_of(jnp.where(real, sc_ref[1, first + e] + off, spare_row), ALIGN), TILE)
            buf[at, 0:d] = gate * out
            buf[at, d:2 * d] = din
            dgb[at, :] = jnp.broadcast_to(jnp.sum(drow * out, axis=1, keepdims=True), (TILE, LANES))
        return carry

    lax.fori_loop(0, (total + TOKEN_UNROLL - 1) // TOKEN_UNROLL, tiles, 0)

    @pl.when(g == pl.num_programs(0) - 1)
    def _():
        lane = lax.broadcasted_iota(jnp.int32, (1, LANES), 1)

        def block(b, carry):
            for k in range(TOKENS_PER_STEP):
                acc, dg = None, jnp.zeros((1, LANES), jnp.float32)
                for j in range(top_k):
                    r = pos_ref[(b * TOKENS_PER_STEP + k) * top_k + j]
                    row = buf[pl.ds(r, 1), :]
                    acc = row if acc is None else acc + row
                    dg = jnp.where(lane == j, dgb[pl.ds(r, 1), :], dg)
                tmp[k:k + 1, :] = acc
                tmpg[k:k + 1, :] = dg
            at = pl.ds(pl.multiple_of(b * TOKENS_PER_STEP, TOKENS_PER_STEP), TOKENS_PER_STEP)
            y_ref[at, :] = (x_ref[at, :].astype(jnp.float32) + tmp[:, 0:d]).astype(jnp.bfloat16)
            dx_ref[at, :] = (dy_ref[at, :].astype(jnp.float32) + tmp[:, d:2 * d]).astype(jnp.bfloat16)
            dg_ref[at, :] = tmpg[...]
            return carry

        lax.fori_loop(0, n_tokens // TOKENS_PER_STEP, block, 0)


def token_pass(scalars, sources, pos, meta, rows, drow, x, dy, w_all, buf_rows, zero_row, top_k):
    n_tokens, d = x.shape
    experts = w_all.shape[0]
    block_rows = meta.shape[0] // sources.shape[0]
    per_dev = experts // sources.shape[0]
    whole = lambda e, *_: (0, 0)
    dest = lambda g, sc, src, pos: (src[g], 0)
    return pl.pallas_call(
        functools.partial(token_kernel, zero_row, top_k),
        out_shape=(jax.ShapeDtypeStruct((n_tokens, d), jnp.bfloat16),
                   jax.ShapeDtypeStruct((n_tokens, d), jnp.bfloat16),
                   jax.ShapeDtypeStruct((n_tokens, LANES), jnp.float32)),
        grid_spec=pltpu.PrefetchScalarGridSpec(
            num_scalar_prefetch=3, grid=(experts // per_dev,),
            in_specs=[pl.BlockSpec((block_rows, 2), dest),
                      pl.BlockSpec((block_rows, d), dest),
                      pl.BlockSpec((block_rows, d), dest),
                      pl.BlockSpec((n_tokens, d), whole, pipeline_mode=pl.Buffered(1)),
                      pl.BlockSpec((n_tokens, d), whole, pipeline_mode=pl.Buffered(1)),
                      pl.BlockSpec((per_dev, *w_all.shape[1:]), lambda g, *_: (g, 0, 0))],
            out_specs=[pl.BlockSpec((n_tokens, d), whole, pipeline_mode=pl.Buffered(1)),
                       pl.BlockSpec((n_tokens, d), whole, pipeline_mode=pl.Buffered(1)),
                       pl.BlockSpec((n_tokens, LANES), whole, pipeline_mode=pl.Buffered(1))],
            scratch_shapes=[pltpu.VMEM((buf_rows, 2 * d), jnp.float32),
                            pltpu.VMEM((buf_rows, LANES), jnp.float32),
                            pltpu.VMEM((TOKENS_PER_STEP, 2 * d), jnp.float32),
                            pltpu.VMEM((TOKENS_PER_STEP, LANES), jnp.float32)]),
        compiler_params=pltpu.CompilerParams(dimension_semantics=("arbitrary",), vmem_limit_bytes=VMEM_BYTES),
        cost_estimate=pl.CostEstimate(flops=40_000_000_000, bytes_accessed=80_000_000, transcendentals=4_000_000),
        name="token_pass",
    )(scalars, sources, pos, meta, rows, drow, x, dy, w_all)


def owner_kernel(sc_ref, meta_ref, xy_ref, w1_ref, w2_ref, dw1_ref, dw2_ref, acc1, acc2, rows_ref, grad_ref):
    s = pl.program_id(0)
    n_tokens = xy_ref.shape[0] // 2
    local_experts = w1_ref.shape[0]

    @pl.when(s == 0)
    def _():
        acc1[...] = jnp.zeros_like(acc1)
        acc2[...] = jnp.zeros_like(acc2)

    last = s * local_experts + local_experts - 1
    used = sc_ref[0, last] + sc_ref[1, last]

    def pick_tile(i, carry):
        at = pl.ds(pl.multiple_of(i * PICK_TILE, PICK_TILE), PICK_TILE)
        meta = meta_ref[at, :]
        pick = pick_matrix(meta, n_tokens)
        rows_ref[at, :] = dot_nn(pick, xy_ref[0:n_tokens, :]).astype(jnp.bfloat16)
        grad_ref[at, :] = (meta[:, 1:2] * dot_nn(pick, xy_ref[n_tokens:, :])).astype(jnp.bfloat16)
        return carry

    lax.fori_loop(0, (used + PICK_TILE - 1) // PICK_TILE, pick_tile, 0)

    first = s * local_experts
    total, find = tile_table([sc_ref[1, first + n] for n in range(local_experts)])

    def tiles(p, carry):
        for u in range(OWNER_UNROLL):
            e, off, count = find(p * OWNER_UNROLL + u)
            at = pl.ds(pl.multiple_of(jnp.where(count > 0, sc_ref[0, first + e] + off, 0), ALIGN), TILE)
            live = lax.broadcasted_iota(jnp.int32, (TILE, 1), 0) < count
            rows = rows_ref[at, :]
            grad = jnp.where(live, grad_ref[at, :].astype(jnp.float32), 0.0).astype(jnp.bfloat16)
            act, slope = gelu_parts(dot_nn(rows, w1_ref[e]))
            dact = dot_nt(grad, w2_ref[e]).astype(jnp.bfloat16).astype(jnp.float32)
            dpre = jnp.where(live, dact * slope, 0.0).astype(jnp.bfloat16)
            act = jnp.where(live, act, 0.0).astype(jnp.bfloat16)
            rows = jnp.where(live, rows.astype(jnp.float32), 0.0).astype(jnp.bfloat16)
            acc2[e] += dot_tn(act, grad)
            acc1[e] += dot_tn(rows, dpre)
        return carry

    lax.fori_loop(0, (total + OWNER_UNROLL - 1) // OWNER_UNROLL, tiles, 0)

    @pl.when(s == pl.num_programs(0) - 1)
    def _():
        dw1_ref[...] = acc1[...].astype(jnp.bfloat16)
        dw2_ref[...] = acc2[...].astype(jnp.bfloat16)


def owner_pass(scalars, meta, xy_all, w1, w2, sources):
    _, d, _ = w1.shape
    block_rows = meta.shape[0] // sources
    return pl.pallas_call(
        owner_kernel,
        out_shape=(jax.ShapeDtypeStruct(w1.shape, jnp.bfloat16), jax.ShapeDtypeStruct(w2.shape, jnp.bfloat16)),
        grid_spec=pltpu.PrefetchScalarGridSpec(
            num_scalar_prefetch=1, grid=(sources,),
            in_specs=[pl.BlockSpec((block_rows, 2), lambda s, *_: (s, 0)),
                      pl.BlockSpec((xy_all.shape[0] // sources, d), lambda s, *_: (s, 0)),
                      pl.BlockSpec(w1.shape, lambda s, *_: (0, 0, 0)),
                      pl.BlockSpec(w2.shape, lambda s, *_: (0, 0, 0))],
            out_specs=[pl.BlockSpec(w1.shape, lambda s, *_: (0, 0, 0)),
                       pl.BlockSpec(w2.shape, lambda s, *_: (0, 0, 0))],
            scratch_shapes=[pltpu.VMEM(w1.shape, jnp.float32), pltpu.VMEM(w2.shape, jnp.float32),
                            pltpu.VMEM((block_rows, d), jnp.bfloat16), pltpu.VMEM((block_rows, d), jnp.bfloat16)]),
        compiler_params=pltpu.CompilerParams(dimension_semantics=("arbitrary",), vmem_limit_bytes=VMEM_BYTES // 2),
        cost_estimate=pl.CostEstimate(flops=60_000_000_000, bytes_accessed=50_000_000, transcendentals=3_000_000),
        name="owner_pass",
    )(scalars, meta, xy_all, w1, w2)


def split3(v):
    a = lax.reduce_precision(v, 8, 7)
    b = lax.reduce_precision(v - a, 8, 7)
    return a, b, lax.reduce_precision(v - a - b, 8, 7)


def route(expert_idx, gate, num_experts, groups, list_rows):
    n_tokens, top_k = expert_idx.shape
    n_pairs = n_tokens * top_k
    local_experts = num_experts // groups
    chunk = 256
    flat = expert_idx.reshape(n_pairs)
    hot = (flat[:, None] == jnp.arange(num_experts, dtype=jnp.int32)[None, :])
    hot_b = hot.astype(jnp.bfloat16).reshape(n_pairs // chunk, chunk, num_experts)
    lower = jnp.tril(jnp.ones((chunk, chunk), jnp.bfloat16), -1)
    inner = jnp.einsum('ij,bje->bie', lower, hot_b, preferred_element_type=jnp.float32)
    sums = jnp.sum(hot_b.astype(jnp.float32), axis=1)
    through = jnp.cumsum(sums, axis=0)
    ranks = inner + (through - sums)[:, None, :]
    counts = through[-1].astype(jnp.int32)
    padded = (counts + ALIGN - 1) // ALIGN * ALIGN
    grid = padded.reshape(groups, local_experts)
    local_start = (jnp.cumsum(grid, axis=1) - grid).reshape(num_experts)
    list_start = local_start + jnp.repeat(jnp.arange(groups, dtype=jnp.int32) * list_rows, local_experts)
    rank = jnp.sum(hot_b.astype(jnp.float32) * ranks, axis=2).reshape(n_pairs).astype(jnp.int32)
    start_of = jnp.sum(jnp.where(hot, list_start[None, :], 0), axis=1)
    list_pos = start_of + rank
    hi = (list_pos[:, None] // LANES == jnp.arange(groups * list_rows // LANES, dtype=jnp.int32)[None, :]).astype(jnp.bfloat16)
    lo = list_pos[:, None] % LANES == jnp.arange(LANES, dtype=jnp.int32)[None, :]
    token = jnp.arange(n_pairs, dtype=jnp.int32) // top_k
    parts = [(token // 32).astype(jnp.float32), (token % 32).astype(jnp.float32), *split3(gate.reshape(n_pairs))]
    vals = jnp.concatenate([jnp.where(lo, v[:, None], 0.0).astype(jnp.bfloat16) for v in parts], axis=1)
    lists = lax.dot_general(hi, vals, (((0,), (0,)), ((), ())), preferred_element_type=jnp.float32)
    t_hi, t_lo, g1, g2, g3 = (lists[:, k * LANES:(k + 1) * LANES] for k in range(5))
    return flat, hot, rank, counts, padded, local_start, 32.0 * t_hi + t_lo, g1 + g2 + g3


def columns(tokens, gates):
    return jnp.stack([tokens.reshape(-1), gates.reshape(-1)], axis=1)


def solution(mesh):
    groups = mesh.shape['expert']
    tok_spec = P(('data', 'expert'), None)
    weight_spec = P('expert', None, None)
    grad_spec = P(('data', 'expert'), None, None)

    def device_pass(x_in, expert_idx, gate_weight, grad_y, w_in, w_out):
        n_tokens, top_k = expert_idx.shape
        local_experts = w_in.shape[0]
        num_experts = local_experts * groups
        n_pairs = n_tokens * top_k
        capacity = (CAP_NUM * n_pairs * groups) // (CAP_DEN * num_experts)
        pair_cap = PAIR_FACTOR * n_pairs // groups
        list_rows = ceil_to(pair_cap + local_experts * (ALIGN - 1) + TILE, LANES)
        me = lax.axis_index('expert')

        d_ff = w_in.shape[2]
        xy = jnp.concatenate([x_in, grad_y], axis=0)
        xy_all = lax.all_gather(xy, 'expert', axis=0, tiled=True)
        w_all = jnp.concatenate([w_in, w_out[:, :, 0:d_ff], w_out[:, :, d_ff:]], axis=1)

        _, hot, rank, counts, padded, local_start, tok_list, gate_list = route(
            expert_idx, gate_weight, num_experts, groups, list_rows)
        count_plane = jnp.zeros((list_rows // LANES, LANES), jnp.float32).at[0, 0:num_experts].set(counts.astype(jnp.float32))
        lists = jnp.stack([tok_list.reshape(groups, -1, LANES), gate_list.reshape(groups, -1, LANES),
                           jnp.broadcast_to(count_plane, (groups, *count_plane.shape))], axis=1)
        lists = lax.all_to_all(lists, 'expert', 0, 0, tiled=True)
        counts_all = lists[:, 2, 0, 0:num_experts].astype(jnp.int32)
        before = jnp.cumsum(counts_all, axis=0) - counts_all
        kept_all = jnp.clip(capacity - before, 0, counts_all)
        kept_mine = lax.dynamic_index_in_dim(kept_all, me, 0, keepdims=False)

        meta = columns(tok_list, gate_list)
        used = jnp.sum(padded.reshape(groups, local_experts), axis=1)
        rows, drow = pick_pass(used, meta, x_in, grad_y)

        w_all = lax.all_gather(w_all, 'expert', axis=0, tiled=True)
        buf_start = jnp.cumsum(padded) - padded
        zero_row = n_pairs + num_experts * (ALIGN - 1) + TILE
        zero_row = ceil_to(zero_row, ALIGN)
        buf_rows = zero_row + ALIGN + TILE
        pick = lambda v: jnp.sum(jnp.where(hot, v[None, :], 0), axis=1)
        pos = jnp.where(rank < pick(kept_mine), pick(buf_start) + rank, zero_row)
        token_scalars = jnp.stack([local_start, buf_start, kept_mine])

        grid_all = ((counts_all + ALIGN - 1) // ALIGN * ALIGN).reshape(groups, groups, local_experts)
        start_all = jnp.cumsum(grid_all, axis=2) - grid_all
        start_own = lax.dynamic_index_in_dim(start_all, me, 1, keepdims=False).reshape(-1)
        kept_own = lax.dynamic_index_in_dim(kept_all.reshape(groups, groups, local_experts), me, 1, keepdims=False).reshape(-1)
        grad_w_in, grad_w_out = owner_pass(jnp.stack([start_own, kept_own]), columns(lists[:, 0], lists[:, 1]),
                                           xy_all, w_in, w_out, groups)
        sources = jnp.arange(groups, dtype=jnp.int32)
        y_out, grad_x, grad_gate = token_pass(token_scalars, sources, pos, meta, rows, drow,
                                              x_in, grad_y, w_all, buf_rows, zero_row, top_k)
        return y_out, grad_x, grad_gate[:, :top_k], grad_w_in, grad_w_out

    return jax.shard_map(device_pass, mesh=mesh,
                         in_specs=(tok_spec, tok_spec, tok_spec, tok_spec, weight_spec, weight_spec),
                         out_specs=(tok_spec, tok_spec, tok_spec, grad_spec, grad_spec), check_vma=False)
```

```python
import functools

import jax
import jax.numpy as jnp
from jax import lax
from jax.experimental import pallas as pl
from jax.experimental.pallas import tpu as pltpu
from jax.sharding import PartitionSpec as P


CAP_NUM = 5
CAP_DEN = 4
PAIR_FACTOR = 2

TILE = 128
PICK_TILE = 256
TOKEN_UNROLL = 2
OWNER_TILE = 256
MOVE_ROWS = 64
ALIGN = 16
LANES = 128
TOKENS_PER_STEP = 16
VMEM_BYTES = 62 * 1024 * 1024
GELU_C = 0.7978845608028654
GELU_K = 0.044715


def ceil_to(n, m):
    return (n + m - 1) // m * m


def gelu_parts(a):
    sq = a * a
    t = jnp.tanh(GELU_C * (a + GELU_K * (sq * a)))
    cdf = 0.5 * (1.0 + t)
    slope = cdf + (0.5 * a) * (1.0 - t * t) * (GELU_C * (1.0 + (3.0 * GELU_K) * sq))
    return a * cdf, slope


def dot_nn(a, b):
    return jnp.dot(a, b, preferred_element_type=jnp.float32)


def dot_nt(a, b):
    return lax.dot_general(a, b, (((1,), (1,)), ((), ())), preferred_element_type=jnp.float32)


def dot_tn(a, b):
    return lax.dot_general(a, b, (((0,), (0,)), ((), ())), preferred_element_type=jnp.float32)


def pick_matrix(meta, n_tokens):
    tok = meta[:, 0:1].astype(jnp.int32)
    cols = lax.broadcasted_iota(jnp.int32, (meta.shape[0], n_tokens), 1)
    return jnp.where(tok == cols, 1.0, 0.0).astype(jnp.bfloat16)


def pick_kernel(n_ref, meta_ref, x_ref, dy_ref, rows_ref, drow_ref):
    used = n_ref[pl.program_id(0)]

    def tile(i, carry):
        at = pl.ds(pl.multiple_of(i * PICK_TILE, PICK_TILE), PICK_TILE)
        pick = pick_matrix(meta_ref[at, :], x_ref.shape[0])
        rows_ref[at, :] = dot_nn(pick, x_ref[...]).astype(jnp.bfloat16)
        drow_ref[at, :] = dot_nn(pick, dy_ref[...]).astype(jnp.bfloat16)
        return carry

    lax.fori_loop(0, (used + PICK_TILE - 1) // PICK_TILE, tile, 0)


def pick_pass(used, meta, x, dy):
    n_tokens, d = x.shape
    dests = used.shape[0]
    block_rows = meta.shape[0] // dests
    whole = lambda e, *_: (0, 0)
    row = lambda e, *_: (e, 0)
    out = jax.ShapeDtypeStruct((meta.shape[0], d), jnp.bfloat16)
    return pl.pallas_call(
        pick_kernel,
        out_shape=(out, out),
        grid_spec=pltpu.PrefetchScalarGridSpec(
            num_scalar_prefetch=1, grid=(dests,),
            in_specs=[pl.BlockSpec((block_rows, 2), row),
                      pl.BlockSpec((n_tokens, d), whole), pl.BlockSpec((n_tokens, d), whole)],
            out_specs=[pl.BlockSpec((block_rows, d), row), pl.BlockSpec((block_rows, d), row)]),
        compiler_params=pltpu.CompilerParams(dimension_semantics=("arbitrary",), vmem_limit_bytes=VMEM_BYTES // 2),
        cost_estimate=pl.CostEstimate(flops=20_000_000_000, bytes_accessed=50_000_000, transcendentals=0),
        name="pick_pass",
    )(used, meta, x, dy)


def out_product(act, w):
    f = w.shape[1]
    d = 2 * f
    return jnp.concatenate([dot_nn(act, w[d:d + f, :]), dot_nn(act, w[d + f:d + 2 * f, :])], axis=1)


def out_product_t(grad, w):
    f = w.shape[1]
    d = 2 * f
    return dot_nt(grad[:, 0:f], w[d:d + f, :]) + dot_nt(grad[:, f:d], w[d + f:d + 2 * f, :])


def tile_table(kept):
    ends, total = [], 0
    for k in kept:
        total = total + (k + TILE - 1) // TILE
        ends.append(total)

    def find(i):
        e, base, live_from = jnp.int32(0), jnp.int32(0), kept[0]
        for n in range(1, len(kept)):
            past = i >= ends[n - 1]
            e = jnp.where(past, n, e)
            base = jnp.where(past, ends[n - 1], base)
            live_from = jnp.where(past, kept[n], live_from)
        off = (i - base) * TILE
        return e, off, live_from - off

    return total, find


def token_kernel(zero_row, top_k, slots, sc_ref, src_ref, pos_ref, meta_ref, rows_ref, drow_ref, x_ref, dy_ref, *refs):
    w_refs, (y_ref, dx_ref, dg_ref, buf, dgb, tmp, tmpg, held, sems) = refs[:2 * slots], refs[2 * slots:]
    g = pl.program_id(0)
    n_tokens, d = x_ref.shape
    half = held.shape[1] // 2
    local_experts = 2 * half

    def fetch(k, h):
        return pltpu.make_async_copy(w_refs[2 * k + h], held.at[k % 2, pl.ds(h * half, half)], sems.at[k % 2, h])

    @pl.when(g == 0)
    def _():
        for h in range(2):
            fetch(0, h).start()

    for k in range(slots):
        @pl.when(g == k)
        def _(k=k):
            if k + 1 < slots:
                for h in range(2):
                    fetch(k + 1, h).start()
            for h in range(2):
                fetch(k, h).wait()

    w_ref = held.at[g % 2]
    spare_row = zero_row + ALIGN

    @pl.when(g == 0)
    def _():
        buf[pl.ds(zero_row, ALIGN), :] = jnp.zeros((ALIGN, 2 * d), jnp.float32)
        dgb[pl.ds(zero_row, ALIGN), :] = jnp.zeros((ALIGN, LANES), jnp.float32)

    first = g * local_experts
    total, find = tile_table([sc_ref[2, first + n] for n in range(local_experts)])

    def tiles(p, carry):
        for u in range(TOKEN_UNROLL):
            e, off, live = find(p * TOKEN_UNROLL + u)
            real = live > 0
            at = pl.ds(pl.multiple_of(jnp.where(real, sc_ref[0, first + e] + off, 0), ALIGN), TILE)
            w = w_ref.at[e]
            gate = meta_ref[at, 1:2]
            drow = drow_ref[at, :].astype(jnp.float32)
            act, slope = gelu_parts(dot_nn(rows_ref[at, :], w[0:d, :]))
            out = out_product(act.astype(jnp.bfloat16), w).astype(jnp.bfloat16).astype(jnp.float32)
            grad = (gate * drow).astype(jnp.bfloat16)
            dact = out_product_t(grad, w).astype(jnp.bfloat16).astype(jnp.float32)
            dpre = (dact * slope).astype(jnp.bfloat16)
            din = dot_nt(dpre, w[0:d, :]).astype(jnp.bfloat16).astype(jnp.float32)
            at = pl.ds(pl.multiple_of(jnp.where(real, sc_ref[1, first + e] + off, spare_row), ALIGN), TILE)
            buf[at, 0:d] = gate * out
            buf[at, d:2 * d] = din
            dgb[at, :] = jnp.broadcast_to(jnp.sum(drow * out, axis=1, keepdims=True), (TILE, LANES))
        return carry

    lax.fori_loop(0, (total + TOKEN_UNROLL - 1) // TOKEN_UNROLL, tiles, 0)

    @pl.when(g == pl.num_programs(0) - 1)
    def _():
        lane = lax.broadcasted_iota(jnp.int32, (1, LANES), 1)

        def block(b, carry):
            for k in range(TOKENS_PER_STEP):
                acc, dg = None, jnp.zeros((1, LANES), jnp.float32)
                for j in range(top_k):
                    r = pos_ref[(b * TOKENS_PER_STEP + k) * top_k + j]
                    row = buf[pl.ds(r, 1), :]
                    acc = row if acc is None else acc + row
                    dg = jnp.where(lane == j, dgb[pl.ds(r, 1), :], dg)
                tmp[k:k + 1, :] = acc
                tmpg[k:k + 1, :] = dg
            at = pl.ds(pl.multiple_of(b * TOKENS_PER_STEP, TOKENS_PER_STEP), TOKENS_PER_STEP)
            y_ref[at, :] = (x_ref[at, :].astype(jnp.float32) + tmp[:, 0:d]).astype(jnp.bfloat16)
            dx_ref[at, :] = (dy_ref[at, :].astype(jnp.float32) + tmp[:, d:2 * d]).astype(jnp.bfloat16)
            dg_ref[at, :] = tmpg[...]
            return carry

        lax.fori_loop(0, n_tokens // TOKENS_PER_STEP, block, 0)


def token_pass(scalars, sources, pos, meta, rows, drow, x, dy, halves, buf_rows, zero_row, top_k):
    n_tokens, d = x.shape
    slots = len(halves)
    half_shape = halves[0][0].shape
    block_rows = meta.shape[0] // slots
    whole = lambda e, *_: (0, 0)
    dest = lambda g, sc, src, pos: (src[g], 0)
    return pl.pallas_call(
        functools.partial(token_kernel, zero_row, top_k, slots),
        out_shape=(jax.ShapeDtypeStruct((n_tokens, d), jnp.bfloat16),
                   jax.ShapeDtypeStruct((n_tokens, d), jnp.bfloat16),
                   jax.ShapeDtypeStruct((n_tokens, LANES), jnp.float32)),
        grid_spec=pltpu.PrefetchScalarGridSpec(
            num_scalar_prefetch=3, grid=(slots,),
            in_specs=[pl.BlockSpec((block_rows, 2), dest),
                      pl.BlockSpec((block_rows, d), dest),
                      pl.BlockSpec((block_rows, d), dest),
                      pl.BlockSpec((n_tokens, d), whole, pipeline_mode=pl.Buffered(1)),
                      pl.BlockSpec((n_tokens, d), whole, pipeline_mode=pl.Buffered(1)),
                      *[pl.BlockSpec(memory_space=pl.ANY)] * (2 * slots)],
            out_specs=[pl.BlockSpec((n_tokens, d), whole, pipeline_mode=pl.Buffered(1)),
                       pl.BlockSpec((n_tokens, d), whole, pipeline_mode=pl.Buffered(1)),
                       pl.BlockSpec((n_tokens, LANES), whole, pipeline_mode=pl.Buffered(1))],
            scratch_shapes=[pltpu.VMEM((buf_rows, 2 * d), jnp.float32),
                            pltpu.VMEM((buf_rows, LANES), jnp.float32),
                            pltpu.VMEM((TOKENS_PER_STEP, 2 * d), jnp.float32),
                            pltpu.VMEM((TOKENS_PER_STEP, LANES), jnp.float32),
                            pltpu.VMEM((2, 2 * half_shape[0], *half_shape[1:]), jnp.bfloat16),
                            pltpu.SemaphoreType.DMA((2, 2))]),
        compiler_params=pltpu.CompilerParams(dimension_semantics=("arbitrary",), vmem_limit_bytes=VMEM_BYTES),
        cost_estimate=pl.CostEstimate(flops=40_000_000_000, bytes_accessed=80_000_000, transcendentals=4_000_000),
        name="token_pass",
    )(scalars, sources, pos, meta, rows, drow, x, dy, *[h for pair in halves for h in pair])


def owner_kernel(sc_ref, meta_ref, xy_ref, w1_ref, w2_ref, dw1_ref, dw2_ref, rows_ref, grad_ref, all_rows, all_grad,
                 acc1, acc2):
    s = pl.program_id(0)
    d = xy_ref.shape[1]
    n_tokens = xy_ref.shape[0] // 2
    local_experts = w1_ref.shape[0]

    last = s * local_experts + local_experts - 1
    used = sc_ref[0, last] + sc_ref[1, last]

    def pick_tile(i, carry):
        at = pl.ds(pl.multiple_of(i * PICK_TILE, PICK_TILE), PICK_TILE)
        meta = meta_ref[at, :]
        pick = pick_matrix(meta, n_tokens)
        rows_ref[at, :] = dot_nn(pick, xy_ref[0:n_tokens, :]).astype(jnp.bfloat16)
        grad_ref[at, :] = (meta[:, 1:2] * dot_nn(pick, xy_ref[n_tokens:, :])).astype(jnp.bfloat16)
        return carry

    lax.fori_loop(0, (used + PICK_TILE - 1) // PICK_TILE, pick_tile, 0)

    for e in range(local_experts):
        start, kept, base = (sc_ref[k, s * local_experts + e] for k in range(3))

        def move(i, carry, e=e, start=start, kept=kept, base=base):
            frm = pl.ds(pl.multiple_of(start + i * MOVE_ROWS, ALIGN), MOVE_ROWS)
            to = pl.ds(pl.multiple_of(base + i * MOVE_ROWS, ALIGN), MOVE_ROWS)
            live = lax.broadcasted_iota(jnp.int32, (MOVE_ROWS, 1), 0) + i * MOVE_ROWS < kept
            all_rows[e, to, :] = jnp.where(live, rows_ref[frm, :], jnp.bfloat16(0))
            all_grad[e, to, :] = jnp.where(live, grad_ref[frm, :], jnp.bfloat16(0))
            return carry

        lax.fori_loop(0, (kept + MOVE_ROWS - 1) // MOVE_ROWS, move, 0)

    @pl.when(s == pl.num_programs(0) - 1)
    def _():
        for e in range(local_experts):
            count = (sc_ref[1, last - local_experts + 1 + e] + ALIGN - 1) // ALIGN * ALIGN
            end = sc_ref[2, last - local_experts + 1 + e] + count

            def clear(i, carry, e=e, end=end):
                to = pl.ds(pl.multiple_of(end + i * MOVE_ROWS, ALIGN), MOVE_ROWS)
                all_rows[e, to, :] = jnp.zeros((MOVE_ROWS, d), jnp.bfloat16)
                all_grad[e, to, :] = jnp.zeros((MOVE_ROWS, d), jnp.bfloat16)
                return carry

            lax.fori_loop(0, OWNER_TILE // MOVE_ROWS, clear, 0)
            acc1[...] = jnp.zeros_like(acc1)
            acc2[...] = jnp.zeros_like(acc2)

            def tile(i, carry, e=e):
                at = pl.ds(pl.multiple_of(i * OWNER_TILE, OWNER_TILE), OWNER_TILE)
                rows, grad = all_rows[e, at, :], all_grad[e, at, :]
                act, slope = gelu_parts(dot_nn(rows, w1_ref[e]))
                dact = dot_nt(grad, w2_ref[e]).astype(jnp.bfloat16).astype(jnp.float32)
                acc2[...] += dot_tn(act.astype(jnp.bfloat16), grad)
                acc1[...] += dot_tn(rows, (dact * slope).astype(jnp.bfloat16))
                return carry

            lax.fori_loop(0, (end + OWNER_TILE - 1) // OWNER_TILE, tile, 0)
            dw1_ref[e] = acc1[...].astype(jnp.bfloat16)
            dw2_ref[e] = acc2[...].astype(jnp.bfloat16)


def owner_pass(scalars, meta, xy_all, w1, w2, sources, capacity):
    local_experts, d, _ = w1.shape
    block_rows = meta.shape[0] // sources
    all_rows = ceil_to(capacity + sources * ALIGN + OWNER_TILE, OWNER_TILE)
    return pl.pallas_call(
        owner_kernel,
        out_shape=(jax.ShapeDtypeStruct(w1.shape, jnp.bfloat16), jax.ShapeDtypeStruct(w2.shape, jnp.bfloat16)),
        grid_spec=pltpu.PrefetchScalarGridSpec(
            num_scalar_prefetch=1, grid=(sources,),
            in_specs=[pl.BlockSpec((block_rows, 2), lambda s, *_: (s, 0)),
                      pl.BlockSpec((xy_all.shape[0] // sources, d), lambda s, *_: (s, 0)),
                      pl.BlockSpec(w1.shape, lambda s, *_: (0, 0, 0)),
                      pl.BlockSpec(w2.shape, lambda s, *_: (0, 0, 0))],
            out_specs=[pl.BlockSpec(w1.shape, lambda s, *_: (0, 0, 0)),
                       pl.BlockSpec(w2.shape, lambda s, *_: (0, 0, 0))],
            scratch_shapes=[pltpu.VMEM((block_rows, d), jnp.bfloat16), pltpu.VMEM((block_rows, d), jnp.bfloat16),
                            pltpu.VMEM((local_experts, all_rows, d), jnp.bfloat16),
                            pltpu.VMEM((local_experts, all_rows, d), jnp.bfloat16),
                            pltpu.VMEM(w1.shape[1:], jnp.float32), pltpu.VMEM(w2.shape[1:], jnp.float32)]),
        compiler_params=pltpu.CompilerParams(dimension_semantics=("arbitrary",), vmem_limit_bytes=VMEM_BYTES),
        cost_estimate=pl.CostEstimate(flops=60_000_000_000, bytes_accessed=50_000_000, transcendentals=3_000_000),
        name="owner_pass",
    )(scalars, meta, xy_all, w1, w2)


def split3(v):
    a = lax.reduce_precision(v, 8, 7)
    b = lax.reduce_precision(v - a, 8, 7)
    return a, b, lax.reduce_precision(v - a - b, 8, 7)


def route(expert_idx, gate, num_experts, groups, list_rows):
    n_tokens, top_k = expert_idx.shape
    n_pairs = n_tokens * top_k
    local_experts = num_experts // groups
    chunk = 256
    flat = expert_idx.reshape(n_pairs)
    hot = (flat[:, None] == jnp.arange(num_experts, dtype=jnp.int32)[None, :])
    hot_b = hot.astype(jnp.bfloat16).reshape(n_pairs // chunk, chunk, num_experts)
    lower = jnp.tril(jnp.ones((chunk, chunk), jnp.bfloat16), -1)
    inner = jnp.einsum('ij,bje->bie', lower, hot_b, preferred_element_type=jnp.float32)
    sums = jnp.sum(hot_b.astype(jnp.float32), axis=1)
    through = jnp.cumsum(sums, axis=0)
    ranks = inner + (through - sums)[:, None, :]
    counts = through[-1].astype(jnp.int32)
    padded = (counts + ALIGN - 1) // ALIGN * ALIGN
    grid = padded.reshape(groups, local_experts)
    local_start = (jnp.cumsum(grid, axis=1) - grid).reshape(num_experts)
    list_start = local_start + jnp.repeat(jnp.arange(groups, dtype=jnp.int32) * list_rows, local_experts)
    rank = jnp.sum(hot_b.astype(jnp.float32) * ranks, axis=2).reshape(n_pairs).astype(jnp.int32)
    start_of = jnp.sum(jnp.where(hot, list_start[None, :], 0), axis=1)
    list_pos = start_of + rank
    hi = (list_pos[:, None] // LANES == jnp.arange(groups * list_rows // LANES, dtype=jnp.int32)[None, :]).astype(jnp.bfloat16)
    lo = list_pos[:, None] % LANES == jnp.arange(LANES, dtype=jnp.int32)[None, :]
    token = jnp.arange(n_pairs, dtype=jnp.int32) // top_k
    parts = [(token // 32).astype(jnp.float32), (token % 32).astype(jnp.float32), *split3(gate.reshape(n_pairs))]
    vals = jnp.concatenate([jnp.where(lo, v[:, None], 0.0).astype(jnp.bfloat16) for v in parts], axis=1)
    lists = lax.dot_general(hi, vals, (((0,), (0,)), ((), ())), preferred_element_type=jnp.float32)
    t_hi, t_lo, g1, g2, g3 = (lists[:, k * LANES:(k + 1) * LANES] for k in range(5))
    return flat, hot, rank, counts, padded, local_start, 32.0 * t_hi + t_lo, g1 + g2 + g3


def columns(tokens, gates):
    return jnp.stack([tokens.reshape(-1), gates.reshape(-1)], axis=1)


def mesh_moves(z_size, y_size):
    cores = 2
    size = z_size * y_size * cores

    def along(move):
        pairs = []
        for i in range(size):
            z, y, c = move(i // (y_size * cores), (i // cores) % y_size, i % cores)
            pairs.append((i, (z * y_size + y) * cores + c))
        return lambda v: lax.ppermute(v, 'expert', pairs)

    z_by = {k: along(lambda z, y, c, k=k: ((z + k) % z_size, y, c)) for k in range(1, z_size)}
    y_swap = along(lambda z, y, c: (z, 1 - y, c))
    c_swap = along(lambda z, y, c: (z, y, 1 - c))
    return z_by, y_swap, c_swap, lambda v: lax.ppermute(v, 'data', [(0, 1), (1, 0)])


def solution(mesh):
    groups = mesh.shape['expert']
    tok_spec = P(('data', 'expert'), None)
    weight_spec = P('expert', None, None)
    grad_spec = P(('data', 'expert'), None, None)

    def device_pass(x_in, expert_idx, gate_weight, grad_y, w_in, w_out):
        n_tokens, top_k = expert_idx.shape
        local_experts = w_in.shape[0]
        num_experts = local_experts * groups
        n_pairs = n_tokens * top_k
        capacity = (CAP_NUM * n_pairs * groups) // (CAP_DEN * num_experts)
        pair_cap = PAIR_FACTOR * n_pairs // groups
        list_rows = ceil_to(pair_cap + local_experts * (ALIGN - 1) + TILE, LANES)
        me = lax.axis_index('expert')

        d_ff = w_in.shape[2]
        half = local_experts // 2
        my_data = lax.axis_index('data')
        w_own = jnp.concatenate([w_in, w_out[:, :, 0:d_ff], w_out[:, :, d_ff:]], axis=1)
        ring = lax.dynamic_slice_in_dim(w_own, my_data * half, half, axis=0)
        other = lax.dynamic_slice_in_dim(w_own, (1 - my_data) * half, half, axis=0)
        z_by, y_swap, c_swap, x_swap = mesh_moves(groups // 4, 2)
        near, z1, z3 = y_swap(ring), z_by[1](ring), z_by[3](ring)
        _, hot, rank, counts, padded, local_start, tok_list, gate_list = route(
            expert_idx, gate_weight, num_experts, groups, list_rows)
        near, z1, z3, ring_late, tok_list, gate_list = lax.optimization_barrier((near, z1, z3, ring, tok_list, gate_list))
        z2 = z_by[2](ring_late)
        near_x = x_swap(near)
        z1_x = x_swap(z1)
        z3_x = x_swap(z3)
        z1_y, z3_y = y_swap(z1), y_swap(z3)
        xy = jnp.concatenate([x_in, grad_y], axis=0)

        count_plane = jnp.zeros((list_rows // LANES, LANES), jnp.float32).at[0, 0:num_experts].set(counts.astype(jnp.float32))
        lists = jnp.stack([tok_list.reshape(groups, -1, LANES), gate_list.reshape(groups, -1, LANES),
                           jnp.broadcast_to(count_plane, (groups, *count_plane.shape))], axis=1)
        lists = lax.all_to_all(lists, 'expert', 0, 0, tiled=True)
        counts_all = lists[:, 2, 0, 0:num_experts].astype(jnp.int32)
        before = jnp.cumsum(counts_all, axis=0) - counts_all
        kept_all = jnp.clip(capacity - before, 0, counts_all)
        kept_mine = lax.dynamic_index_in_dim(kept_all, me, 0, keepdims=False)

        meta = columns(tok_list, gate_list)
        used = jnp.sum(padded.reshape(groups, local_experts), axis=1)
        rows, drow = pick_pass(used, meta, x_in, grad_y)
        z1_y, z3_y, z2, rows, drow = lax.optimization_barrier((z1_y, z3_y, z2, rows, drow))
        z2_y = y_swap(z2)
        xy, _ = lax.optimization_barrier((xy, rows))
        xy_all = lax.all_gather(xy, 'expert', axis=0, tiled=True)
        halves, where = [], []
        for at, v, u in [((0, 0), ring, other), ((0, 1), near, near_x), ((1, 0), z1, z1_x), ((3, 0), z3, z3_x),
                         ((1, 1), z1_y, x_swap(z1_y)), ((3, 1), z3_y, x_swap(z3_y)),
                         ((2, 0), z2, x_swap(z2)), ((2, 1), z2_y, x_swap(z2_y))]:
            halves += [(v, u), (c_swap(v), c_swap(u))]
            where += [(*at, 0), (*at, 1)]

        z, y, c = me // 4, (me // 2) % 2, me % 2
        sources = jnp.stack([((z - dz) % 4) * 4 + (y ^ dy) * 2 + (c ^ dc) for dz, dy, dc in where]).astype(jnp.int32)
        order = (sources[:, None] * local_experts
                 + (jnp.arange(local_experts, dtype=jnp.int32) + half * my_data) % local_experts).reshape(num_experts)
        slot_hot = order[:, None] == jnp.arange(num_experts, dtype=jnp.int32)[None, :]
        by_slot = lambda v: jnp.sum(jnp.where(slot_hot, v[None, :], 0), axis=1)
        padded_slot = by_slot(padded)
        slot_start = jnp.cumsum(padded_slot) - padded_slot
        buf_start = jnp.sum(jnp.where(slot_hot, slot_start[:, None], 0), axis=0)
        zero_row = n_pairs + num_experts * (ALIGN - 1) + TILE
        zero_row = ceil_to(zero_row, ALIGN)
        buf_rows = zero_row + ALIGN + TILE
        pick = lambda v: jnp.sum(jnp.where(hot, v[None, :], 0), axis=1)
        pos = jnp.where(rank < pick(kept_mine), pick(buf_start) + rank, zero_row)
        token_scalars = jnp.stack([by_slot(local_start), slot_start, by_slot(kept_mine)])

        grid_all = ((counts_all + ALIGN - 1) // ALIGN * ALIGN).reshape(groups, groups, local_experts)
        start_all = jnp.cumsum(grid_all, axis=2) - grid_all
        start_own = lax.dynamic_index_in_dim(start_all, me, 1, keepdims=False).reshape(-1)
        kept_own = lax.dynamic_index_in_dim(kept_all.reshape(groups, groups, local_experts), me, 1, keepdims=False).reshape(-1)
        kept_rows = (kept_own.reshape(groups, local_experts) + ALIGN - 1) // ALIGN * ALIGN
        base_own = (jnp.cumsum(kept_rows, axis=0) - kept_rows).reshape(-1)
        grad_w_in, grad_w_out = owner_pass(jnp.stack([start_own, kept_own, base_own]), columns(lists[:, 0], lists[:, 1]),
                                           xy_all, w_in, w_out, groups, capacity)
        y_out, grad_x, grad_gate = token_pass(token_scalars, sources, pos, meta, rows, drow,
                                              x_in, grad_y, halves, buf_rows, zero_row, top_k)
        return y_out, grad_x, grad_gate[:, :top_k], grad_w_in, grad_w_out

    return jax.shard_map(device_pass, mesh=mesh,
                         in_specs=(tok_spec, tok_spec, tok_spec, tok_spec, weight_spec, weight_spec),
                         out_specs=(tok_spec, tok_spec, tok_spec, grad_spec, grad_spec), check_vma=False)
```

```python
import functools

import jax
import jax.numpy as jnp
from jax import lax
from jax.experimental import pallas as pl
from jax.experimental.pallas import tpu as pltpu
from jax.sharding import PartitionSpec as P


CAP_NUM = 5
CAP_DEN = 4
PAIR_FACTOR = 2

TILE = 128
PICK_TILE = 256
TOKEN_UNROLL = 2
OWNER_TILE = 512
MOVE_ROWS = 64
ALIGN = 16
LANES = 128
TOKENS_PER_STEP = 16
VMEM_BYTES = 62 * 1024 * 1024
GELU_C = 0.7978845608028654
GELU_K = 0.044715


def ceil_to(n, m):
    return (n + m - 1) // m * m


def gelu_parts(a):
    sq = a * a
    t = jnp.tanh(GELU_C * (a + GELU_K * (sq * a)))
    cdf = 0.5 * (1.0 + t)
    slope = cdf + (0.5 * a) * (1.0 - t * t) * (GELU_C * (1.0 + (3.0 * GELU_K) * sq))
    return a * cdf, slope


def dot_nn(a, b):
    return jnp.dot(a, b, preferred_element_type=jnp.float32)


def dot_nt(a, b):
    return lax.dot_general(a, b, (((1,), (1,)), ((), ())), preferred_element_type=jnp.float32)


def dot_tn(a, b):
    return lax.dot_general(a, b, (((0,), (0,)), ((), ())), preferred_element_type=jnp.float32)


def pick_matrix(meta, n_tokens):
    tok = meta[:, 0:1].astype(jnp.int32)
    cols = lax.broadcasted_iota(jnp.int32, (meta.shape[0], n_tokens), 1)
    return jnp.where(tok == cols, 1.0, 0.0).astype(jnp.bfloat16)


def pick_kernel(first, n_ref, meta_ref, x_ref, dy_ref, *refs):
    rows_ref, drow_ref = refs[-2:]
    used = n_ref[first + pl.program_id(0)]

    def tile(i, carry):
        at = pl.ds(pl.multiple_of(i * PICK_TILE, PICK_TILE), PICK_TILE)
        pick = pick_matrix(meta_ref[at, :], x_ref.shape[0])
        rows_ref[at, :] = dot_nn(pick, x_ref[...]).astype(jnp.bfloat16)
        drow_ref[at, :] = dot_nn(pick, dy_ref[...]).astype(jnp.bfloat16)
        return carry

    lax.fori_loop(0, (used + PICK_TILE - 1) // PICK_TILE, tile, 0)


def pick_pass(used, meta, x, dy, first, count, into=()):
    n_tokens, d = x.shape
    block_rows = meta.shape[0] // used.shape[0]
    whole = lambda e, *_: (0, 0)
    row = lambda e, *_: (first + e, 0)
    out = jax.ShapeDtypeStruct((meta.shape[0], d), jnp.bfloat16)
    return pl.pallas_call(
        functools.partial(pick_kernel, first),
        out_shape=(out, out),
        grid_spec=pltpu.PrefetchScalarGridSpec(
            num_scalar_prefetch=1, grid=(count,),
            in_specs=[pl.BlockSpec((block_rows, 2), row),
                      pl.BlockSpec((n_tokens, d), whole), pl.BlockSpec((n_tokens, d), whole),
                      *[pl.BlockSpec(memory_space=pl.ANY) for _ in into]],
            out_specs=[pl.BlockSpec((block_rows, d), row), pl.BlockSpec((block_rows, d), row)]),
        compiler_params=pltpu.CompilerParams(dimension_semantics=("arbitrary",), vmem_limit_bytes=VMEM_BYTES // 2),
        input_output_aliases={4 + k: k for k in range(len(into))},
        cost_estimate=pl.CostEstimate(flops=10_000_000_000, bytes_accessed=25_000_000, transcendentals=0),
        name="pick_pass",
    )(used, meta, x, dy, *into)


def out_product(act, w):
    f = w.shape[1]
    d = 2 * f
    return jnp.concatenate([dot_nn(act, w[d:d + f, :]), dot_nn(act, w[d + f:d + 2 * f, :])], axis=1)


def out_product_t(grad, w):
    f = w.shape[1]
    d = 2 * f
    return dot_nt(grad[:, 0:f], w[d:d + f, :]) + dot_nt(grad[:, f:d], w[d + f:d + 2 * f, :])


def tile_table(kept):
    ends, total = [], 0
    for k in kept:
        total = total + (k + TILE - 1) // TILE
        ends.append(total)

    def find(i):
        e, base, live_from = jnp.int32(0), jnp.int32(0), kept[0]
        for n in range(1, len(kept)):
            past = i >= ends[n - 1]
            e = jnp.where(past, n, e)
            base = jnp.where(past, ends[n - 1], base)
            live_from = jnp.where(past, kept[n], live_from)
        off = (i - base) * TILE
        return e, off, live_from - off

    return total, find


def token_kernel(zero_row, top_k, slots, sc_ref, src_ref, pos_ref, meta_ref, rows_ref, drow_ref, x_ref, dy_ref, *refs):
    w_refs, (y_ref, dx_ref, dg_ref, buf, dgb, tmp, tmpg, held, sems) = refs[:2 * slots], refs[2 * slots:]
    g = pl.program_id(0)
    n_tokens, d = x_ref.shape
    half = held.shape[1] // 2
    local_experts = 2 * half

    def fetch(k, h):
        return pltpu.make_async_copy(w_refs[2 * k + h], held.at[k % 2, pl.ds(h * half, half)], sems.at[k % 2, h])

    @pl.when(g == 0)
    def _():
        for h in range(2):
            fetch(0, h).start()

    for k in range(slots):
        @pl.when(g == k)
        def _(k=k):
            if k + 1 < slots:
                for h in range(2):
                    fetch(k + 1, h).start()
            for h in range(2):
                fetch(k, h).wait()

    w_ref = held.at[g % 2]
    spare_row = zero_row + ALIGN

    @pl.when(g == 0)
    def _():
        buf[pl.ds(zero_row, ALIGN), :] = jnp.zeros((ALIGN, 2 * d), jnp.float32)
        dgb[pl.ds(zero_row, ALIGN), :] = jnp.zeros((ALIGN, LANES), jnp.float32)

    first = g * local_experts
    total, find = tile_table([sc_ref[2, first + n] for n in range(local_experts)])

    def tiles(p, carry):
        for u in range(TOKEN_UNROLL):
            e, off, live = find(p * TOKEN_UNROLL + u)
            real = live > 0
            at = pl.ds(pl.multiple_of(jnp.where(real, sc_ref[0, first + e] + off, 0), ALIGN), TILE)
            w = w_ref.at[e]
            gate = meta_ref[at, 1:2]
            drow = drow_ref[at, :].astype(jnp.float32)
            act, slope = gelu_parts(dot_nn(rows_ref[at, :], w[0:d, :]))
            out = out_product(act.astype(jnp.bfloat16), w).astype(jnp.bfloat16).astype(jnp.float32)
            grad = (gate * drow).astype(jnp.bfloat16)
            dact = out_product_t(grad, w).astype(jnp.bfloat16).astype(jnp.float32)
            dpre = (dact * slope).astype(jnp.bfloat16)
            din = dot_nt(dpre, w[0:d, :]).astype(jnp.bfloat16).astype(jnp.float32)
            at = pl.ds(pl.multiple_of(jnp.where(real, sc_ref[1, first + e] + off, spare_row), ALIGN), TILE)
            buf[at, 0:d] = gate * out
            buf[at, d:2 * d] = din
            dgb[at, :] = jnp.broadcast_to(jnp.sum(drow * out, axis=1, keepdims=True), (TILE, LANES))
        return carry

    lax.fori_loop(0, (total + TOKEN_UNROLL - 1) // TOKEN_UNROLL, tiles, 0)

    @pl.when(g == pl.num_programs(0) - 1)
    def _():
        lane = lax.broadcasted_iota(jnp.int32, (1, LANES), 1)

        def block(b, carry):
            for k in range(TOKENS_PER_STEP):
                acc, dg = None, jnp.zeros((1, LANES), jnp.float32)
                for j in range(top_k):
                    r = pos_ref[(b * TOKENS_PER_STEP + k) * top_k + j]
                    row = buf[pl.ds(r, 1), :]
                    acc = row if acc is None else acc + row
                    dg = jnp.where(lane == j, dgb[pl.ds(r, 1), :], dg)
                tmp[k:k + 1, :] = acc
                tmpg[k:k + 1, :] = dg
            at = pl.ds(pl.multiple_of(b * TOKENS_PER_STEP, TOKENS_PER_STEP), TOKENS_PER_STEP)
            y_ref[at, :] = (x_ref[at, :].astype(jnp.float32) + tmp[:, 0:d]).astype(jnp.bfloat16)
            dx_ref[at, :] = (dy_ref[at, :].astype(jnp.float32) + tmp[:, d:2 * d]).astype(jnp.bfloat16)
            dg_ref[at, :] = tmpg[...]
            return carry

        lax.fori_loop(0, n_tokens // TOKENS_PER_STEP, block, 0)


def token_pass(scalars, sources, pos, meta, rows, drow, x, dy, halves, buf_rows, zero_row, top_k):
    n_tokens, d = x.shape
    slots = len(halves)
    half_shape = halves[0][0].shape
    block_rows = meta.shape[0] // slots
    whole = lambda e, *_: (0, 0)
    dest = lambda g, sc, src, pos: (src[g], 0)
    return pl.pallas_call(
        functools.partial(token_kernel, zero_row, top_k, slots),
        out_shape=(jax.ShapeDtypeStruct((n_tokens, d), jnp.bfloat16),
                   jax.ShapeDtypeStruct((n_tokens, d), jnp.bfloat16),
                   jax.ShapeDtypeStruct((n_tokens, LANES), jnp.float32)),
        grid_spec=pltpu.PrefetchScalarGridSpec(
            num_scalar_prefetch=3, grid=(slots,),
            in_specs=[pl.BlockSpec((block_rows, 2), dest),
                      pl.BlockSpec((block_rows, d), dest),
                      pl.BlockSpec((block_rows, d), dest),
                      pl.BlockSpec((n_tokens, d), whole, pipeline_mode=pl.Buffered(1)),
                      pl.BlockSpec((n_tokens, d), whole, pipeline_mode=pl.Buffered(1)),
                      *[pl.BlockSpec(memory_space=pl.ANY)] * (2 * slots)],
            out_specs=[pl.BlockSpec((n_tokens, d), whole, pipeline_mode=pl.Buffered(1)),
                       pl.BlockSpec((n_tokens, d), whole, pipeline_mode=pl.Buffered(1)),
                       pl.BlockSpec((n_tokens, LANES), whole, pipeline_mode=pl.Buffered(1))],
            scratch_shapes=[pltpu.VMEM((buf_rows, 2 * d), jnp.float32),
                            pltpu.VMEM((buf_rows, LANES), jnp.float32),
                            pltpu.VMEM((TOKENS_PER_STEP, 2 * d), jnp.float32),
                            pltpu.VMEM((TOKENS_PER_STEP, LANES), jnp.float32),
                            pltpu.VMEM((2, 2 * half_shape[0], *half_shape[1:]), jnp.bfloat16),
                            pltpu.SemaphoreType.DMA((2, 2))]),
        compiler_params=pltpu.CompilerParams(dimension_semantics=("arbitrary",), vmem_limit_bytes=VMEM_BYTES),
        cost_estimate=pl.CostEstimate(flops=40_000_000_000, bytes_accessed=80_000_000, transcendentals=4_000_000),
        name="token_pass",
    )(scalars, sources, pos, meta, rows, drow, x, dy, *[h for pair in halves for h in pair])


def owner_kernel(sc_ref, meta_ref, xy_ref, w1_ref, w2_ref, dw1_ref, dw2_ref, rows_ref, grad_ref, all_rows, all_grad,
                 acc1, acc2):
    s = pl.program_id(0)
    d = xy_ref.shape[1]
    n_tokens = xy_ref.shape[0] // 2
    local_experts = w1_ref.shape[0]

    last = s * local_experts + local_experts - 1
    used = sc_ref[0, last] + sc_ref[1, last]

    def pick_tile(i, carry):
        at = pl.ds(pl.multiple_of(i * PICK_TILE, PICK_TILE), PICK_TILE)
        meta = meta_ref[at, :]
        pick = pick_matrix(meta, n_tokens)
        rows_ref[at, :] = dot_nn(pick, xy_ref[0:n_tokens, :]).astype(jnp.bfloat16)
        grad_ref[at, :] = (meta[:, 1:2] * dot_nn(pick, xy_ref[n_tokens:, :])).astype(jnp.bfloat16)
        return carry

    lax.fori_loop(0, (used + PICK_TILE - 1) // PICK_TILE, pick_tile, 0)

    for e in range(local_experts):
        start, kept, base = (sc_ref[k, s * local_experts + e] for k in range(3))

        def move(i, carry, e=e, start=start, kept=kept, base=base):
            frm = pl.ds(pl.multiple_of(start + i * MOVE_ROWS, ALIGN), MOVE_ROWS)
            to = pl.ds(pl.multiple_of(base + i * MOVE_ROWS, ALIGN), MOVE_ROWS)
            live = lax.broadcasted_iota(jnp.int32, (MOVE_ROWS, 1), 0) + i * MOVE_ROWS < kept
            all_rows[e, to, :] = jnp.where(live, rows_ref[frm, :], jnp.bfloat16(0))
            all_grad[e, to, :] = jnp.where(live, grad_ref[frm, :], jnp.bfloat16(0))
            return carry

        lax.fori_loop(0, (kept + MOVE_ROWS - 1) // MOVE_ROWS, move, 0)

    @pl.when(s == pl.num_programs(0) - 1)
    def _():
        for e in range(local_experts):
            count = (sc_ref[1, last - local_experts + 1 + e] + ALIGN - 1) // ALIGN * ALIGN
            end = sc_ref[2, last - local_experts + 1 + e] + count

            def clear(i, carry, e=e, end=end):
                to = pl.ds(pl.multiple_of(end + i * MOVE_ROWS, ALIGN), MOVE_ROWS)
                all_rows[e, to, :] = jnp.zeros((MOVE_ROWS, d), jnp.bfloat16)
                all_grad[e, to, :] = jnp.zeros((MOVE_ROWS, d), jnp.bfloat16)
                return carry

            lax.fori_loop(0, OWNER_TILE // MOVE_ROWS, clear, 0)
            acc1[...] = jnp.zeros_like(acc1)
            acc2[...] = jnp.zeros_like(acc2)

            def tile(i, carry, e=e):
                at = pl.ds(pl.multiple_of(i * OWNER_TILE, OWNER_TILE), OWNER_TILE)
                rows, grad = all_rows[e, at, :], all_grad[e, at, :]
                act, slope = gelu_parts(dot_nn(rows, w1_ref[e]))
                dact = dot_nt(grad, w2_ref[e]).astype(jnp.bfloat16).astype(jnp.float32)
                acc2[...] += dot_tn(act.astype(jnp.bfloat16), grad)
                acc1[...] += dot_tn(rows, (dact * slope).astype(jnp.bfloat16))
                return carry

            lax.fori_loop(0, (end + OWNER_TILE - 1) // OWNER_TILE, tile, 0)
            dw1_ref[e] = acc1[...].astype(jnp.bfloat16)
            dw2_ref[e] = acc2[...].astype(jnp.bfloat16)


def owner_pass(scalars, meta, xy_all, w1, w2, sources, capacity):
    local_experts, d, _ = w1.shape
    block_rows = meta.shape[0] // sources
    all_rows = ceil_to(capacity + sources * ALIGN + OWNER_TILE, OWNER_TILE)
    return pl.pallas_call(
        owner_kernel,
        out_shape=(jax.ShapeDtypeStruct(w1.shape, jnp.bfloat16), jax.ShapeDtypeStruct(w2.shape, jnp.bfloat16)),
        grid_spec=pltpu.PrefetchScalarGridSpec(
            num_scalar_prefetch=1, grid=(sources,),
            in_specs=[pl.BlockSpec((block_rows, 2), lambda s, *_: (s, 0)),
                      pl.BlockSpec((xy_all.shape[0] // sources, d), lambda s, *_: (s, 0)),
                      pl.BlockSpec(w1.shape, lambda s, *_: (0, 0, 0)),
                      pl.BlockSpec(w2.shape, lambda s, *_: (0, 0, 0))],
            out_specs=[pl.BlockSpec(w1.shape, lambda s, *_: (0, 0, 0)),
                       pl.BlockSpec(w2.shape, lambda s, *_: (0, 0, 0))],
            scratch_shapes=[pltpu.VMEM((block_rows, d), jnp.bfloat16), pltpu.VMEM((block_rows, d), jnp.bfloat16),
                            pltpu.VMEM((local_experts, all_rows, d), jnp.bfloat16),
                            pltpu.VMEM((local_experts, all_rows, d), jnp.bfloat16),
                            pltpu.VMEM(w1.shape[1:], jnp.float32), pltpu.VMEM(w2.shape[1:], jnp.float32)]),
        compiler_params=pltpu.CompilerParams(dimension_semantics=("arbitrary",), vmem_limit_bytes=VMEM_BYTES),
        cost_estimate=pl.CostEstimate(flops=60_000_000_000, bytes_accessed=50_000_000, transcendentals=3_000_000),
        name="owner_pass",
    )(scalars, meta, xy_all, w1, w2)


def split3(v):
    a = lax.reduce_precision(v, 8, 7)
    b = lax.reduce_precision(v - a, 8, 7)
    return a, b, lax.reduce_precision(v - a - b, 8, 7)


def route(expert_idx, gate, num_experts, groups, list_rows, hold):
    n_tokens, top_k = expert_idx.shape
    n_pairs = n_tokens * top_k
    local_experts = num_experts // groups
    chunk = 256
    flat = expert_idx.reshape(n_pairs)
    hot = (flat[:, None] == jnp.arange(num_experts, dtype=jnp.int32)[None, :])
    hot_b = hot.astype(jnp.bfloat16).reshape(n_pairs // chunk, chunk, num_experts)
    lower = jnp.tril(jnp.ones((chunk, chunk), jnp.bfloat16), -1)
    inner = jnp.einsum('ij,bje->bie', lower, hot_b, preferred_element_type=jnp.float32)
    sums = jnp.sum(hot_b.astype(jnp.float32), axis=1)
    through = jnp.cumsum(sums, axis=0)
    ranks = inner + (through - sums)[:, None, :]
    counts = through[-1].astype(jnp.int32)
    padded = (counts + ALIGN - 1) // ALIGN * ALIGN
    grid = padded.reshape(groups, local_experts)
    local_start = (jnp.cumsum(grid, axis=1) - grid).reshape(num_experts)
    list_start = local_start + jnp.repeat(jnp.arange(groups, dtype=jnp.int32) * list_rows, local_experts)
    rank = jnp.sum(hot_b.astype(jnp.float32) * ranks, axis=2).reshape(n_pairs).astype(jnp.int32)
    start_of = jnp.sum(jnp.where(hot, list_start[None, :], 0), axis=1)
    list_pos = start_of + rank
    hi = (list_pos[:, None] // LANES == jnp.arange(groups * list_rows // LANES, dtype=jnp.int32)[None, :]).astype(jnp.bfloat16)
    lo = list_pos[:, None] % LANES == jnp.arange(LANES, dtype=jnp.int32)[None, :]
    token = jnp.arange(n_pairs, dtype=jnp.int32) // top_k
    parts = [(token // 32).astype(jnp.float32), (token % 32).astype(jnp.float32), *split3(gate.reshape(n_pairs))]
    vals = jnp.concatenate([jnp.where(lo, v[:, None], 0.0).astype(jnp.bfloat16) for v in parts], axis=1)
    vals, *hold = lax.optimization_barrier((vals, *hold))
    lists = lax.dot_general(hi, vals, (((0,), (0,)), ((), ())), preferred_element_type=jnp.float32)
    t_hi, t_lo, g1, g2, g3 = (lists[:, k * LANES:(k + 1) * LANES] for k in range(5))
    return flat, hot, rank, counts, padded, local_start, 32.0 * t_hi + t_lo, g1 + g2 + g3, hold


def columns(tokens, gates):
    return jnp.stack([tokens.reshape(-1), gates.reshape(-1)], axis=1)


def mesh_moves(z_size, y_size):
    cores = 2
    size = z_size * y_size * cores

    def along(move):
        pairs = []
        for i in range(size):
            z, y, c = move(i // (y_size * cores), (i // cores) % y_size, i % cores)
            pairs.append((i, (z * y_size + y) * cores + c))
        return lambda v: lax.ppermute(v, 'expert', pairs)

    z_by = {k: along(lambda z, y, c, k=k: ((z + k) % z_size, y, c)) for k in range(1, z_size)}
    y_swap = along(lambda z, y, c: (z, 1 - y, c))
    c_swap = along(lambda z, y, c: (z, y, 1 - c))
    return z_by, y_swap, c_swap, lambda v: lax.ppermute(v, 'data', [(0, 1), (1, 0)])


def solution(mesh):
    groups = mesh.shape['expert']
    tok_spec = P(('data', 'expert'), None)
    weight_spec = P('expert', None, None)
    grad_spec = P(('data', 'expert'), None, None)

    def device_pass(x_in, expert_idx, gate_weight, grad_y, w_in, w_out):
        n_tokens, top_k = expert_idx.shape
        local_experts = w_in.shape[0]
        num_experts = local_experts * groups
        n_pairs = n_tokens * top_k
        capacity = (CAP_NUM * n_pairs * groups) // (CAP_DEN * num_experts)
        pair_cap = PAIR_FACTOR * n_pairs // groups
        list_rows = ceil_to(pair_cap + local_experts * (ALIGN - 1) + TILE, LANES)
        me = lax.axis_index('expert')

        d_ff = w_in.shape[2]
        half = local_experts // 2
        my_data = lax.axis_index('data')
        w_own = jnp.concatenate([w_in, w_out[:, :, 0:d_ff], w_out[:, :, d_ff:]], axis=1)
        ring = lax.dynamic_slice_in_dim(w_own, my_data * half, half, axis=0)
        other = lax.dynamic_slice_in_dim(w_own, (1 - my_data) * half, half, axis=0)
        z_by, y_swap, c_swap, x_swap = mesh_moves(groups // 4, 2)
        near, z1, z3 = y_swap(ring), z_by[1](ring), z_by[3](ring)
        flat, hot, rank, counts, padded, local_start, tok_list, gate_list, (near, ring_late) = route(
            expert_idx, gate_weight, num_experts, groups, list_rows, (near, ring))
        z2 = z_by[2](ring_late)
        near_x = x_swap(near)

        meta = columns(tok_list, gate_list)
        used = jnp.sum(padded.reshape(groups, local_experts), axis=1)
        z1, z3, used, meta = lax.optimization_barrier((z1, z3, used, meta))
        z1_y = y_swap(z1)
        z3_y = y_swap(z3)
        z1_x = x_swap(z1)
        z3_x = x_swap(z3)
        z2_y = y_swap(z2)
        z2_x = x_swap(z2)
        xy = jnp.concatenate([x_in, grad_y], axis=0)
        z1_y, z3_y, xy = lax.optimization_barrier((z1_y, z3_y, xy))
        xy_all = lax.all_gather(xy, 'expert', axis=0, tiled=True)
        z1_yx = x_swap(z1_y)
        z3_yx = x_swap(z3_y)
        z2_y, used = lax.optimization_barrier((z2_y, used))
        z2_yx = x_swap(z2_y)
        rows, drow = pick_pass(used, meta, x_in, grad_y, 0, groups)
        count_plane = jnp.zeros((list_rows // LANES, LANES), jnp.float32).at[0, 0:num_experts].set(counts.astype(jnp.float32))
        lists = jnp.stack([tok_list.reshape(groups, -1, LANES), gate_list.reshape(groups, -1, LANES),
                           jnp.broadcast_to(count_plane, (groups, *count_plane.shape))], axis=1)
        lists, _ = lax.optimization_barrier((lists, rows))
        lists = lax.all_to_all(lists, 'expert', 0, 0, tiled=True)
        counts_all = lists[:, 2, 0, 0:num_experts].astype(jnp.int32)
        before = jnp.cumsum(counts_all, axis=0) - counts_all
        kept_all = jnp.clip(capacity - before, 0, counts_all)
        kept_mine = lax.dynamic_index_in_dim(kept_all, me, 0, keepdims=False)

        halves, where = [], []
        for at, v, u in [((0, 0), ring, other), ((0, 1), near, near_x), ((1, 0), z1, z1_x), ((3, 0), z3, z3_x),
                         ((1, 1), z1_y, z1_yx), ((3, 1), z3_y, z3_yx),
                         ((2, 0), z2, z2_x), ((2, 1), z2_y, z2_yx)]:
            halves += [(v, u), (c_swap(v), c_swap(u))]
            where += [(*at, 0), (*at, 1)]

        z, y, c = me // 4, (me // 2) % 2, me % 2
        sources = jnp.stack([((z - dz) % 4) * 4 + (y ^ dy) * 2 + (c ^ dc) for dz, dy, dc in where]).astype(jnp.int32)
        order = (sources[:, None] * local_experts
                 + (jnp.arange(local_experts, dtype=jnp.int32) + half * my_data) % local_experts).reshape(num_experts)
        slot_hot = order[:, None] == jnp.arange(num_experts, dtype=jnp.int32)[None, :]
        by_slot = lambda v: jnp.sum(jnp.where(slot_hot, v[None, :], 0), axis=1)
        padded_slot = by_slot(padded)
        slot_start = jnp.cumsum(padded_slot) - padded_slot
        buf_start = jnp.sum(jnp.where(slot_hot, slot_start[:, None], 0), axis=0)
        zero_row = n_pairs + num_experts * (ALIGN - 1) + TILE
        zero_row = ceil_to(zero_row, ALIGN)
        buf_rows = zero_row + ALIGN + TILE
        pick = lambda v: jnp.sum(jnp.where(hot, v[None, :], 0), axis=1)
        pos = jnp.where(rank < pick(kept_mine), pick(buf_start) + rank, zero_row)
        token_scalars = jnp.stack([by_slot(local_start), slot_start, by_slot(kept_mine)])

        grid_all = ((counts_all + ALIGN - 1) // ALIGN * ALIGN).reshape(groups, groups, local_experts)
        start_all = jnp.cumsum(grid_all, axis=2) - grid_all
        start_own = lax.dynamic_index_in_dim(start_all, me, 1, keepdims=False).reshape(-1)
        kept_own = lax.dynamic_index_in_dim(kept_all.reshape(groups, groups, local_experts), me, 1, keepdims=False).reshape(-1)
        kept_rows = (kept_own.reshape(groups, local_experts) + ALIGN - 1) // ALIGN * ALIGN
        base_own = (jnp.cumsum(kept_rows, axis=0) - kept_rows).reshape(-1)
        grad_w_in, grad_w_out = owner_pass(jnp.stack([start_own, kept_own, base_own]), columns(lists[:, 0], lists[:, 1]),
                                           xy_all, w_in, w_out, groups, capacity)
        y_out, grad_x, grad_gate = token_pass(token_scalars, sources, pos, meta, rows, drow,
                                              x_in, grad_y, halves, buf_rows, zero_row, top_k)
        return y_out, grad_x, grad_gate[:, :top_k], grad_w_in, grad_w_out

    return jax.shard_map(device_pass, mesh=mesh,
                         in_specs=(tok_spec, tok_spec, tok_spec, tok_spec, weight_spec, weight_spec),
                         out_specs=(tok_spec, tok_spec, tok_spec, grad_spec, grad_spec), check_vma=False)
```
